32 devices in a mesh: blk: 8 (over z, y), grid: 4 (over x, core).
Axes of the slice: x: 2, y: 2, z: 4, core: 2. Of those that a mesh axis runs over, the one named last changes fastest.
Arguments:
- orbitals: bfloat16 [32, 64, 4096], P('blk', 'grid'), may hold values from -60 to 60
Outputs:
- rotated: bfloat16 [32, 64, 4096], P(None, 'grid', 'blk')
- intersection: float32 [32, 32], replicated
The draws below stay inside these ranges and needn't reach their ends.
All inputs are finite; a program needn't handle non-finite values.
Results may differ from the reference program's by a relative error of at most 0.0085.
Values may be sent and summed in bfloat16 or wider, within the bound.
No kernel may reach another device: no remote copies, remote signals or barrier semaphores. Data moves between devices by JAX's collectives and lax.ppermute only.
A program may use at most 128 MiB of HBM per device.

```python
import jax
import jax.numpy as jnp
from jax import lax

NX = 64
NY = 64
NZ = 64
ORB_DEV = 4
STEPS = 2
ORBITALS = 32
NYZ = 4096
N_BLK = 8
N_GRID = 4


def draw_orbitals(key, part):
    keys = jax.random.split(jax.random.fold_in(key, 17), 6)
    row_scale = jnp.exp(jax.random.uniform(keys[0], (ORBITALS, 1, 1), jnp.float32, jnp.log(0.6), jnp.log(1.9)))
    cell_scale = jnp.exp(jax.random.uniform(keys[1], (1, NX, NY * NZ), jnp.float32, jnp.log(0.6), jnp.log(1.9)))
    slab_rows = NX // N_GRID
    run_cells = NY * NZ // N_BLK
    slab_pick = jax.random.randint(keys[4], (), 0, N_GRID)
    run_pick = jax.random.randint(keys[5], (), 0, N_BLK)
    row_index = jnp.arange(NX, dtype=jnp.int32)[None, :, None]
    cell_index = jnp.arange(NY * NZ, dtype=jnp.int32)[None, None, :]
    inside = (row_index // slab_rows == slab_pick) & (cell_index // run_cells == run_pick)
    heavy = jnp.where(inside, 3.0, 1.0).astype(jnp.float32)
    noise = jax.random.normal(keys[2], (ORBITALS, NX, NY * NZ), jnp.float32)
    values = row_scale * cell_scale * heavy * jnp.clip(noise, -5.0, 5.0)
    return jnp.clip(values, -60.0, 60.0).astype(jnp.bfloat16)


def setup_inputs(seed: int = 0) -> dict:
    key_list = jax.random.split(jax.random.key(seed), 2)
    orbitals = draw_orbitals(jax.random.fold_in(key_list[1], 71), 0)
    return dict(orbitals=orbitals)


exchange_fraction = 0.25
screening = 1.0

def sine_table(length):
    index = jnp.arange(length).astype(jnp.float32)
    angle = jnp.pi * (index[:, None] + 1.0) * (index[None, :] + 1.0) / (length + 1)
    return (jnp.sqrt(2.0 / (length + 1)) * jnp.sin(angle)).astype(jnp.bfloat16)

def eigen_values(length, count):
    index = jnp.arange(count).astype(jnp.float32)
    return 2.0 - 2.0 * jnp.cos(jnp.pi * (index + 1.0) / (length + 1))

def kernel_weights():
    values_x = eigen_values(NX, NX)
    values_y = eigen_values(NY, NY)
    values_z = eigen_values(NZ, NZ)
    return 1.0 / (screening + values_x[:, None, None] + values_y[None, :, None] + values_z[None, None, :])

def along(field, table, form):
    return jnp.einsum(form, field.astype(jnp.float32), table.astype(jnp.float32))

def poisson(density):
    table_x = sine_table(NX)
    table_y = sine_table(NY)
    table_z = sine_table(NZ)
    first = along(density, table_z, 'pxyz,zc->pxyc').astype(jnp.bfloat16)
    modes = along(first, table_y, 'pxyz,yc->pxcz').astype(jnp.bfloat16)
    scaled = (along(modes, table_x, 'pxyz,xc->pcyz') * kernel_weights()).astype(jnp.bfloat16)
    back = along(scaled, table_x, 'pxyz,xc->pcyz').astype(jnp.bfloat16)
    third = along(back, table_y, 'pxyz,yc->pxcz').astype(jnp.bfloat16)
    return along(third, table_z, 'pxyz,zc->pxyc')

def reference(orbitals):
    block_count = ORBITALS // ORB_DEV
    blocks = orbitals.reshape(block_count, ORB_DEV, NX, NY, NZ)

    def per_block(block):
        own_field = lax.dynamic_index_in_dim(blocks, block, 0, keepdims=False)
        sources = []
        for cycle_step in range(1, STEPS + 1):
            index = ((block - cycle_step) % block_count).astype(jnp.int32)
            sources.append(lax.dynamic_index_in_dim(blocks, index, 0, keepdims=False))
        sources = jnp.concatenate(sources, axis=0)

        def add_source(summed, source_field):
            density = (own_field.astype(jnp.float32) * source_field.astype(jnp.float32)[None]).astype(jnp.bfloat16)
            potential = poisson(density)
            return (summed + potential * source_field.astype(jnp.float32)[None], None)
        start = jnp.zeros((ORB_DEV, NX, NY, NZ), jnp.float32)
        summed, discarded = lax.scan(add_source, start, sources)
        return (own_field.astype(jnp.float32) - exchange_fraction * summed).astype(jnp.bfloat16)
    updated = lax.map(per_block, jnp.arange(block_count).astype(jnp.int32))
    flat = updated.reshape(ORBITALS, NX * NY * NZ)
    intersection = jnp.dot(flat.astype(jnp.float32), flat.T.astype(jnp.float32), preferred_element_type=jnp.float32) / (NX * NY * NZ)
    factor = jnp.linalg.cholesky(intersection)
    identity = jnp.eye(ORBITALS, dtype=jnp.float32)
    inverse = jax.scipy.linalg.solve_triangular(factor, identity, lower=True).astype(jnp.bfloat16)
    rotated = jnp.dot(inverse.astype(jnp.float32), flat.astype(jnp.float32), preferred_element_type=jnp.float32).astype(jnp.bfloat16)
    return (rotated.reshape(ORBITALS, NX, NYZ), intersection)
```

```python
import functools

import jax
import jax.numpy as jnp
from jax import lax
from jax.experimental import pallas as pl
from jax.experimental.pallas import tpu as pltpu
from jax.sharding import PartitionSpec as P

NX = 64
NY = 64
NZ = 64
STEPS = 2

exchange_fraction = 0.25
screening = 1.0

BF = jnp.bfloat16
F32 = jnp.float32
VMEM = pl.BlockSpec(memory_space=pltpu.VMEM)
SMEM = pl.BlockSpec(memory_space=pltpu.SMEM)
LANES = 128
ROW_PAD = 8
QUAD = 4
UNROLL = 4


def product(a, b):
    return jnp.dot(a, b, preferred_element_type=F32)


def sine_rows(length, index_in):
    modes = jnp.arange(length).astype(F32)
    angle = jnp.pi * (modes[:, None] + 1.0) * (index_in.astype(F32)[None, :] + 1.0) / (length + 1)
    return (jnp.sqrt(2.0 / (length + 1)) * jnp.sin(angle)).astype(BF)


def block_diagonal(table, copies):
    n = table.shape[0]
    eye = jnp.eye(copies, dtype=BF)
    return (eye[:, None, :, None] * table[None, :, None, :]).reshape(copies * n, copies * n)


def eigen_values(length):
    index = jnp.arange(length).astype(F32)
    return 2.0 - 2.0 * jnp.cos(jnp.pi * (index + 1.0) / (length + 1))


def kernel_weights():
    values_x = eigen_values(NX)
    values_y = eigen_values(NY)
    values_z = eigen_values(NZ)
    weights = 1.0 / (
        screening + values_x[:, None, None] + values_y[None, :, None] + values_z[None, None, :]
    )
    return weights.reshape(NX * NY, NZ)


def block_kernel(slabs, final, rest):
    own = rest[:slabs]
    src = rest[slabs:2 * slabs]
    rest = rest[2 * slabs:]
    pos_ref, tz_ref, tx_ref, txb_ref, ty_ref, w_ref = rest[:6]
    rest = rest[6:]
    if final:
        acc_ref, out_ref, grouped_ref, work_ref = rest
    else:
        out_ref, grouped_ref, work_ref = rest
    count = src[0].shape[0]
    rows = src[0].shape[1]
    halves = count * NZ // LANES
    width = QUAD * NZ
    pitch = work_ref.shape[1] // NY

    def tile(refs, lead, off, size):
        parts = [r[lead + (slice(None), pl.ds(off, size))] for r in refs]
        return jnp.concatenate(parts, 0)

    def load_rows(first):
        parts = []
        for q in range(QUAD):
            at = pl.multiple_of((first + q) * pitch, 8)
            parts.append(
                jnp.concatenate([work_ref[h, pl.ds(at, NX), :] for h in range(halves)], 1)
            )
        return jnp.concatenate(parts, 0)

    def forward(t, carry):
        off = pl.multiple_of(t * width, width)
        at = pl.multiple_of(t * QUAD * NX, QUAD * NX)
        mine = tile(own, (), off, width)
        others = [tile(src, (j,), off, width) for j in range(count)]
        pairs = [mine * other for other in others]
        cut = [slice(q * NZ, (q + 1) * NZ) for q in range(QUAD)]
        density = jnp.concatenate(
            [jnp.concatenate([p[:, c] for p in pairs], 1) for c in cut], 0)
        grouped_ref[pl.ds(at, QUAD * NX), :] = jnp.concatenate(
            [jnp.concatenate([o[:, c] for o in others], 1) for c in cut], 0)
        first = product(density, tz_ref[...]).astype(BF)
        modes = product(tx_ref[...], first)
        for q in range(QUAD):
            to = pl.multiple_of((t * QUAD + q) * pitch, 8)
            for h in range(halves):
                work_ref[h, pl.ds(to, NX), :] = modes[q * NX:(q + 1) * NX, h * LANES:(h + 1) * LANES]
        return carry

    def solve(t, carry):
        at = pl.multiple_of(t * QUAD * NY, QUAD * NY)
        modes = jnp.concatenate([
            jnp.concatenate(
                [work_ref[h, pl.ds(t * QUAD + q, NY, stride=pitch), :] for h in range(halves)], 1)
            for q in range(QUAD)], 0).astype(BF)
        weights = jnp.concatenate([w_ref[pl.ds(at, QUAD * NY), :]] * halves, 1)
        scaled = (product(ty_ref[...], modes) * weights).astype(BF)
        back = product(ty_ref[...], scaled)
        for q in range(QUAD):
            for h in range(halves):
                work_ref[h, pl.ds(t * QUAD + q, NY, stride=pitch), :] = (
                    back[q * NY:(q + 1) * NY, h * LANES:(h + 1) * LANES])
        return carry

    lane = lax.broadcasted_iota(jnp.int32, (NX, LANES), 1)
    per_tile = LANES // NZ

    def backward(t, carry):
        at = pl.multiple_of(t * QUAD * NX, QUAD * NX)
        third = product(txb_ref[...], load_rows(t * QUAD).astype(BF)).astype(BF)
        potential = product(third, tz_ref[...])
        terms = potential * grouped_ref[pl.ds(at, QUAD * NX), :].astype(F32)
        total = terms[:, :LANES]
        for h in range(1, halves):
            total = total + terms[:, h * LANES:(h + 1) * LANES]
        total = total + pltpu.roll(total, NZ, 1)
        for q in range(0, QUAD, per_tile):
            exchange = jnp.where(
                lane < NZ, total[q * NX:(q + 1) * NX], total[(q + 1) * NX:(q + 2) * NX])
            off = pl.multiple_of((t * QUAD + q) * NZ, LANES)
            if not final:
                out_ref[:, pl.ds(off, LANES)] = exchange
                continue
            exchange = exchange + acc_ref[:, pl.ds(off, LANES)]
            mine = tile(own, (), off, LANES).astype(F32)
            updated = (mine - exchange_fraction * exchange).astype(BF)
            for r in range(slabs):
                part = updated[r * rows:(r + 1) * rows]
                if len(out_ref.shape) == 4:
                    share = out_ref.shape[3] // LANES
                    index = (t * QUAD + q) * NZ // LANES
                    to = pl.multiple_of((index % share) * LANES, LANES)
                    out_ref[index // share, pos_ref[r], :, pl.ds(to, LANES)] = part
                else:
                    out_ref[pos_ref[r], :, pl.ds(off, LANES)] = part
        return carry

    lax.fori_loop(0, NY // QUAD, forward, 0, unroll=UNROLL)
    lax.fori_loop(0, NX // QUAD, solve, 0, unroll=UNROLL)
    lax.fori_loop(0, NY // QUAD, backward, 0, unroll=UNROLL)


def add_block(own, src, tables, acc, out_shape):
    slabs = len(own)
    count = src[0].shape[0]
    final = acc is not None
    lead = () if acc is None else (acc,)
    flops = 12 * count * NX * NY * NZ * NZ * 4
    return pl.pallas_call(
        lambda *refs: block_kernel(slabs, final, refs),
        out_shape=out_shape,
        in_specs=[VMEM] * (2 * slabs) + [SMEM] + [VMEM] * (5 + len(lead)),
        out_specs=VMEM,
        scratch_shapes=[
            pltpu.VMEM((NY * NX, count * NZ), BF),
            pltpu.VMEM((count * NZ // LANES, NY * (NX + ROW_PAD), LANES), F32),
        ],
        compiler_params=pltpu.CompilerParams(vmem_limit_bytes=40 * 1024 * 1024),
        cost_estimate=pl.CostEstimate(flops=flops, bytes_accessed=8 << 20, transcendentals=0),
    )(*own, *src, *tables, *lead)


def gram_kernel(x_ref, out_ref):
    orbs, rows, lanes = x_ref.shape
    flat = x_ref[...].reshape(orbs * rows, lanes)
    full = lax.dot_general(flat, flat, (((1,), (1,)), ((), ())), preferred_element_type=F32)
    down = lax.broadcasted_iota(jnp.int32, full.shape, 0)
    along = lax.broadcasted_iota(jnp.int32, full.shape, 1)
    full = jnp.where(down % rows == along % rows, full, 0.0)
    half = jnp.sum(full.reshape(orbs, rows, orbs * rows), axis=1)
    out_ref[...] = jnp.sum(half.T.reshape(orbs, rows, orbs), axis=1)


def rotate_kernel(scale, parts_ref, x_ref, out_ref, gram_ref):
    orbs, rows, lanes = x_ref.shape
    gram = jnp.sum(parts_ref[...], axis=0) * scale
    gram_ref[...] = gram
    down = lax.broadcasted_iota(jnp.int32, (orbs, orbs), 0)
    along = lax.broadcasted_iota(jnp.int32, (orbs, orbs), 1)
    eye = jnp.where(down == along, 1.0, 0.0)
    work = jnp.concatenate([gram, eye], 1)
    row = lax.broadcasted_iota(jnp.int32, (orbs, 1), 0)
    pivots = jnp.zeros((orbs, 1), F32)
    for k in range(orbs):
        column = work[:, k:k + 1]
        pivot = work[k:k + 1, k:k + 1]
        pivots = jnp.where(row == k, pivot, pivots)
        factor = jnp.where(row > k, column / pivot, 0.0)
        work = work - factor * work[k:k + 1, :]
    inverse = (work[:, orbs:] * (1.0 / jnp.sqrt(pivots))).astype(BF)
    tall = lax.broadcasted_iota(jnp.int32, (orbs * rows, orbs), 0) // rows
    wide = lax.broadcasted_iota(jnp.int32, (orbs * rows, orbs), 1)
    pick = jnp.where(tall == wide, 1.0, 0.0).astype(BF)
    spread = product(pick, inverse).astype(BF)
    spread = lax.dot_general(spread, pick, (((1,), (1,)), ((), ())), preferred_element_type=F32)
    i = lax.broadcasted_iota(jnp.int32, spread.shape, 0)
    j = lax.broadcasted_iota(jnp.int32, spread.shape, 1)
    spread = jnp.where(i % rows == j % rows, spread, 0.0).astype(BF)
    flat = x_ref[...].reshape(orbs * rows, lanes)
    out_ref[...] = product(spread, flat).astype(BF).reshape(orbs, rows, lanes)


def exchanged(x, axis, by):
    return lax.ppermute(x, axis, [(i, i ^ by) for i in range(lax.axis_size(axis))])


def gathered(slab):
    size = lax.axis_size("grid")
    slabs = {0: slab}
    bit = size // 2
    while bit:
        for r in list(slabs):
            slabs[r | bit] = exchanged(slabs[r], "grid", bit)
        bit //= 2
    return [slabs[r] for r in range(size)]


def body(orbitals):
    orb_count, slab_rows, plane_cells = orbitals.shape
    slabs = lax.axis_size("grid")
    blocks = lax.axis_size("blk")
    assert orb_count == slabs and slab_rows * slabs == NX and blocks % 2 == 0 and STEPS == 2
    grid_index = lax.axis_index("grid")
    order = jnp.arange(slabs) ^ grid_index

    far = lax.ppermute(orbitals, "blk", [(i, (i + 2) % blocks) for i in range(blocks)])
    own = [lax.dynamic_index_in_dim(orbitals, grid_index, 0, keepdims=False)]
    for r in range(1, slabs):
        piece = lax.dynamic_index_in_dim(orbitals, grid_index ^ r, 0, keepdims=False)
        own.append(exchanged(piece, "grid", r))
    near = exchanged(jnp.where(lax.axis_index("blk") % 2 == 0, orbitals, far), "blk", 1)
    far = gathered(far)
    near = gathered(near)

    cells = jnp.arange(NX)
    here = (order[:, None] * slab_rows + jnp.arange(slab_rows)[None, :]).reshape(NX)
    table_x = sine_rows(NX, here)
    table_z = sine_rows(NZ, cells[:NZ])
    weights = jnp.concatenate([kernel_weights()] * (LANES // NZ), 1)
    tables = (
        order.astype(jnp.int32),
        block_diagonal(table_z, orb_count),
        block_diagonal(table_x, QUAD),
        block_diagonal(table_x.T, QUAD),
        block_diagonal(sine_rows(NY, cells[:NY]), QUAD),
        weights,
    )
    acc = add_block(own, far, tables, None, jax.ShapeDtypeStruct((NX, plane_cells), F32))
    chunk = plane_cells // blocks
    if chunk % LANES == 0:
        shape = (blocks, slabs, slab_rows, chunk)
    else:
        shape = (slabs, slab_rows, plane_cells)
    updated = add_block(own, near, tables, acc, jax.ShapeDtypeStruct(shape, BF))
    if chunk % LANES:
        updated = updated.reshape(slabs, slab_rows, blocks, chunk).transpose(2, 0, 1, 3)
    updated = updated.reshape(blocks * slabs, slab_rows, chunk)
    cellwise = lax.all_to_all(updated, ("blk", "grid"), 0, 0, tiled=True)

    devices = blocks * slabs
    cell_count = NX * NY * NZ
    if devices * slab_rows <= 512 and chunk % LANES == 0:
        local = pl.pallas_call(
            gram_kernel,
            out_shape=jax.ShapeDtypeStruct((devices, devices), F32),
            in_specs=[VMEM],
            out_specs=VMEM,
        )(cellwise)
        parts = lax.all_to_all(
            jnp.broadcast_to(local[None], (devices,) + local.shape), ("blk", "grid"), 0, 0)
        return pl.pallas_call(
            functools.partial(rotate_kernel, 1.0 / cell_count),
            out_shape=(
                jax.ShapeDtypeStruct(cellwise.shape, BF),
                jax.ShapeDtypeStruct(local.shape, F32),
            ),
            in_specs=[VMEM, VMEM],
            out_specs=(VMEM, VMEM),
        )(parts, cellwise)
    flat = cellwise.reshape(devices, slab_rows * chunk)
    local = jnp.dot(flat, flat.T, preferred_element_type=F32)
    intersection = lax.psum(local, ("blk", "grid")) / cell_count
    factor = jnp.linalg.cholesky(intersection)
    identity = jnp.eye(devices, dtype=F32)
    inverse = jax.scipy.linalg.solve_triangular(factor, identity, lower=True).astype(BF)
    rotated = product(inverse, flat).astype(BF)
    return (rotated.reshape(cellwise.shape), intersection)


def solution(mesh):
    in_specs = (P("blk", "grid", None),)
    out_specs = (P(None, "grid", "blk"), P())
    return jax.shard_map(body, mesh=mesh, in_specs=in_specs, out_specs=out_specs, check_vma=False)
```

```python
import functools

import jax
import jax.numpy as jnp
from jax import lax
from jax.experimental import pallas as pl
from jax.experimental.pallas import tpu as pltpu
from jax.sharding import PartitionSpec as P

NX = 64
NY = 64
NZ = 64
STEPS = 2

exchange_fraction = 0.25
screening = 1.0

BF = jnp.bfloat16
F32 = jnp.float32
VMEM = pl.BlockSpec(memory_space=pltpu.VMEM)
SMEM = pl.BlockSpec(memory_space=pltpu.SMEM)
LANES = 128
ROW_PAD = 8
QUAD = 4
UNROLL = 4
PANEL = 8


def product(a, b):
    return jnp.dot(a, b, preferred_element_type=F32)


def sine_tables(rows, columns):
    angle = jnp.pi * (rows[:, :, None] + 1.0) * (columns[:, None, :] + 1.0) / (NX + 1)
    return (jnp.sqrt(2.0 / (NX + 1)) * jnp.sin(angle)).astype(BF)


def eigen_values(length):
    index = jnp.arange(length).astype(F32)
    return 2.0 - 2.0 * jnp.cos(jnp.pi * (index + 1.0) / (length + 1))


def table_kernel(sine_ref, lam_ref, lanes_ref, diag_ref, weight_ref):
    count, n, _ = sine_ref.shape
    size = diag_ref.shape[1]
    down = lax.broadcasted_iota(jnp.int32, (size, size), 0) // n
    along = lax.broadcasted_iota(jnp.int32, (size, size), 1) // n
    for i in range(count):
        table = sine_ref[i].astype(F32)
        table = jnp.concatenate([table] * (size // n), 1)
        table = jnp.concatenate([table] * (size // n), 0)
        diag_ref[i] = jnp.where(down == along, table, 0.0).astype(BF)
    columns = lam_ref[...]
    lanes = lanes_ref[...]
    for k in range(n):
        total = screening + columns[k:k + 1, :] + columns + lanes
        weight_ref[k * n:(k + 1) * n, :] = 1.0 / total


def make_tables(here):
    cells = jnp.arange(NX).astype(F32)
    here = here.astype(F32)
    sine = sine_tables(jnp.stack([cells, cells, here]), jnp.stack([cells, here, cells]))
    lam = eigen_values(NX)
    size = QUAD * NX
    return pl.pallas_call(
        table_kernel,
        out_shape=(
            jax.ShapeDtypeStruct((3, size, size), BF),
            jax.ShapeDtypeStruct((NX * NY, LANES), F32),
        ),
        in_specs=[VMEM] * 3,
        out_specs=(VMEM, VMEM),
        cost_estimate=pl.CostEstimate(flops=1 << 26, bytes_accessed=3 << 20, transcendentals=0),
    )(sine, jnp.broadcast_to(lam[:, None], (NX, LANES)),
      jnp.concatenate([lam] * (LANES // NZ))[None, :])


def block_kernel(slabs, final, rest):
    own = rest[:slabs]
    src = rest[slabs:2 * slabs]
    rest = rest[2 * slabs:]
    pos_ref, tab_ref, w_ref = rest[:3]
    rest = rest[3:]
    if final:
        acc_ref, out_ref, grouped_ref, work_ref = rest
    else:
        out_ref, grouped_ref, work_ref = rest
    count = src[0].shape[0]
    rows = src[0].shape[1]
    halves = count * NZ // LANES
    width = QUAD * NZ
    pitch = work_ref.shape[1] // NY

    def tile(refs, lead, off, size):
        parts = [r[lead + (slice(None), pl.ds(off, size))] for r in refs]
        return jnp.concatenate(parts, 0)

    def load_rows(first):
        parts = []
        for q in range(QUAD):
            at = pl.multiple_of((first + q) * pitch, 8)
            parts.append(
                jnp.concatenate([work_ref[h, pl.ds(at, NX), :] for h in range(halves)], 1)
            )
        return jnp.concatenate(parts, 0)

    def forward(t, carry):
        off = pl.multiple_of(t * width, width)
        at = pl.multiple_of(t * QUAD * NX, QUAD * NX)
        mine = tile(own, (), off, width)
        others = [tile(src, (j,), off, width) for j in range(count)]
        pairs = [mine * other for other in others]
        cut = [slice(q * NZ, (q + 1) * NZ) for q in range(QUAD)]
        density = jnp.concatenate(
            [jnp.concatenate([p[:, c] for p in pairs], 1) for c in cut], 0)
        grouped_ref[pl.ds(at, QUAD * NX), :] = jnp.concatenate(
            [jnp.concatenate([o[:, c] for o in others], 1) for c in cut], 0)
        first = product(density, tab_ref[0]).astype(BF)
        modes = product(tab_ref[1], first)
        for q in range(QUAD):
            to = pl.multiple_of((t * QUAD + q) * pitch, 8)
            for h in range(halves):
                work_ref[h, pl.ds(to, NX), :] = modes[q * NX:(q + 1) * NX, h * LANES:(h + 1) * LANES]
        return carry

    def solve(t, carry):
        at = pl.multiple_of(t * QUAD * NY, QUAD * NY)
        modes = jnp.concatenate([
            jnp.concatenate(
                [work_ref[h, pl.ds(t * QUAD + q, NY, stride=pitch), :] for h in range(halves)], 1)
            for q in range(QUAD)], 0).astype(BF)
        weights = jnp.concatenate([w_ref[pl.ds(at, QUAD * NY), :]] * halves, 1)
        scaled = (product(tab_ref[0], modes) * weights).astype(BF)
        back = product(tab_ref[0], scaled)
        for q in range(QUAD):
            for h in range(halves):
                work_ref[h, pl.ds(t * QUAD + q, NY, stride=pitch), :] = (
                    back[q * NY:(q + 1) * NY, h * LANES:(h + 1) * LANES])
        return carry

    lane = lax.broadcasted_iota(jnp.int32, (NX, LANES), 1)
    per_tile = LANES // NZ

    def backward(t, carry):
        at = pl.multiple_of(t * QUAD * NX, QUAD * NX)
        third = product(tab_ref[2], load_rows(t * QUAD).astype(BF)).astype(BF)
        potential = product(third, tab_ref[0])
        terms = potential * grouped_ref[pl.ds(at, QUAD * NX), :].astype(F32)
        total = terms[:, :LANES]
        for h in range(1, halves):
            total = total + terms[:, h * LANES:(h + 1) * LANES]
        total = total + pltpu.roll(total, NZ, 1)
        for q in range(0, QUAD, per_tile):
            exchange = jnp.where(
                lane < NZ, total[q * NX:(q + 1) * NX], total[(q + 1) * NX:(q + 2) * NX])
            off = pl.multiple_of((t * QUAD + q) * NZ, LANES)
            if not final:
                out_ref[:, pl.ds(off, LANES)] = exchange
                continue
            exchange = exchange + acc_ref[:, pl.ds(off, LANES)]
            mine = tile(own, (), off, LANES).astype(F32)
            updated = (mine - exchange_fraction * exchange).astype(BF)
            for r in range(slabs):
                part = updated[r * rows:(r + 1) * rows]
                if len(out_ref.shape) == 4:
                    share = out_ref.shape[3] // LANES
                    index = (t * QUAD + q) * NZ // LANES
                    to = pl.multiple_of((index % share) * LANES, LANES)
                    out_ref[index // share, pos_ref[r], :, pl.ds(to, LANES)] = part
                else:
                    out_ref[pos_ref[r], :, pl.ds(off, LANES)] = part
        return carry

    lax.fori_loop(0, NY // QUAD, forward, 0, unroll=UNROLL)
    lax.fori_loop(0, NX // QUAD, solve, 0, unroll=UNROLL)
    lax.fori_loop(0, NY // QUAD, backward, 0, unroll=UNROLL)


def add_block(own, src, tables, acc, out_shape):
    slabs = len(own)
    count = src[0].shape[0]
    final = acc is not None
    lead = () if acc is None else (acc,)
    flops = 12 * count * NX * NY * NZ * NZ * 4
    return pl.pallas_call(
        lambda *refs: block_kernel(slabs, final, refs),
        out_shape=out_shape,
        in_specs=[VMEM] * (2 * slabs) + [SMEM] + [VMEM] * (2 + len(lead)),
        out_specs=VMEM,
        scratch_shapes=[
            pltpu.VMEM((NY * NX, count * NZ), BF),
            pltpu.VMEM((count * NZ // LANES, NY * (NX + ROW_PAD), LANES), F32),
        ],
        compiler_params=pltpu.CompilerParams(vmem_limit_bytes=40 * 1024 * 1024),
        cost_estimate=pl.CostEstimate(flops=flops, bytes_accessed=8 << 20, transcendentals=0),
    )(*own, *src, *tables, *lead)


def gram_kernel(x_ref, out_ref):
    orbs, rows, lanes = x_ref.shape
    flat = x_ref[...].reshape(orbs * rows, lanes)
    full = lax.dot_general(flat, flat, (((1,), (1,)), ((), ())), preferred_element_type=F32)
    down = lax.broadcasted_iota(jnp.int32, (rows, orbs * rows), 0)
    along = lax.broadcasted_iota(jnp.int32, (rows, orbs * rows), 1)
    same = down == along % rows
    half = [
        jnp.sum(jnp.where(same, full[o * rows:(o + 1) * rows], 0.0), axis=0, keepdims=True)
        for o in range(orbs)
    ]
    half = jnp.concatenate(half, 0)
    gram = jnp.sum(half.T.reshape(orbs, rows, orbs), axis=1)
    deep = orbs * orbs // LANES
    packed = jnp.concatenate([gram[q * deep:(q + 1) * deep] for q in range(orbs // deep)], 1)
    out_ref[...] = jnp.broadcast_to(packed[None], out_ref.shape)


def rotate_kernel(scale, parts_ref, x_ref, out_ref, gram_ref):
    orbs, rows, lanes = x_ref.shape
    packed = jnp.sum(parts_ref[...], axis=0) * scale
    deep = packed.shape[0]
    gram = jnp.concatenate(
        [packed[:, q * orbs:(q + 1) * orbs] for q in range(LANES // orbs)], 0)
    gram_ref[...] = gram
    down = lax.broadcasted_iota(jnp.int32, (orbs, orbs), 0)
    along = lax.broadcasted_iota(jnp.int32, (orbs, orbs), 1)
    eye = jnp.where(down == along, 1.0, 0.0)
    zero = jnp.zeros((orbs, LANES - 2 * orbs), F32)
    work = jnp.concatenate([gram, eye, zero], 1)
    row = lax.broadcasted_iota(jnp.int32, (orbs, LANES), 0)
    pivots = jnp.zeros((orbs, LANES), F32)
    for first in range(0, orbs, PANEL):
        columns = [
            jnp.broadcast_to(work[:, c:c + 1], (orbs, LANES)) for c in range(first, first + PANEL)
        ]
        for k in range(first, first + PANEL):
            column = columns[k - first]
            pivot = column[k:k + 1, :]
            pivots = jnp.where(row == k, pivot, pivots)
            factor = jnp.where(row > k, column * (1.0 / pivot), 0.0)
            work = work - factor * work[k:k + 1, :]
            for c in range(k - first + 1, PANEL):
                columns[c] = columns[c] - factor * columns[c][k:k + 1, :]
    work = work * (1.0 / jnp.sqrt(pivots))
    inverse = work[:, orbs:2 * orbs].astype(BF)
    tall = lax.broadcasted_iota(jnp.int32, (orbs * rows, orbs), 0) // rows
    wide = lax.broadcasted_iota(jnp.int32, (orbs * rows, orbs), 1)
    pick = jnp.where(tall == wide, 1.0, 0.0).astype(BF)
    spread = product(pick, inverse).astype(BF)
    spread = lax.dot_general(spread, pick, (((1,), (1,)), ((), ())), preferred_element_type=F32)
    i = lax.broadcasted_iota(jnp.int32, (orbs * rows, 1), 0) % rows
    j = lax.broadcasted_iota(jnp.int32, (1, orbs * rows), 1) % rows
    spread = jnp.where(i == j, spread, 0.0).astype(BF)
    flat = x_ref[...].reshape(orbs * rows, lanes)
    out_ref[...] = product(spread, flat).astype(BF).reshape(orbs, rows, lanes)


def exchanged(x, axis, by):
    return lax.ppermute(x, axis, [(i, i ^ by) for i in range(lax.axis_size(axis))])


def gathered(slab, after=None):
    size = lax.axis_size("grid")
    slabs = {0: slab}
    bit = size // 2
    while bit:
        for r in list(slabs):
            source = slabs[r]
            if after is not None and bit == 1 and r == size - 2:
                source, after = lax.optimization_barrier((source, after))
                slabs[r] = source
            slabs[r | bit] = exchanged(source, "grid", bit)
        bit //= 2
    slabs = [slabs[r] for r in range(size)]
    return slabs if after is None else (slabs, after)


def body(orbitals):
    orb_count, slab_rows, plane_cells = orbitals.shape
    slabs = lax.axis_size("grid")
    blocks = lax.axis_size("blk")
    assert orb_count == slabs and slab_rows * slabs == NX and blocks % 2 == 0 and STEPS == 2
    grid_index = lax.axis_index("grid")
    order = jnp.arange(slabs) ^ grid_index

    here = (order[:, None] * slab_rows + jnp.arange(slab_rows)[None, :]).reshape(NX)
    diagonals, weights = make_tables(here)

    far = lax.ppermute(orbitals, "blk", [(i, (i + 2) % blocks) for i in range(blocks)])
    own = [lax.dynamic_index_in_dim(orbitals, grid_index, 0, keepdims=False)]
    for r in range(1, slabs):
        piece = lax.dynamic_index_in_dim(orbitals, grid_index ^ r, 0, keepdims=False)
        own.append(exchanged(piece, "grid", r))
    relay = jnp.where(lax.axis_index("blk") % 2 == 0, orbitals, far)
    relay, diagonals, weights, own = lax.optimization_barrier((relay, diagonals, weights, own))
    tables = (order.astype(jnp.int32), diagonals, weights)
    near = exchanged(relay, "blk", 1)
    far = gathered(far)
    acc = add_block(own, far, tables, None, jax.ShapeDtypeStruct((NX, plane_cells), F32))
    near, acc = gathered(near, acc)
    chunk = plane_cells // blocks
    if chunk % LANES == 0:
        shape = (blocks, slabs, slab_rows, chunk)
    else:
        shape = (slabs, slab_rows, plane_cells)
    updated = add_block(own, near, tables, acc, jax.ShapeDtypeStruct(shape, BF))
    if chunk % LANES:
        updated = updated.reshape(slabs, slab_rows, blocks, chunk).transpose(2, 0, 1, 3)
    updated = updated.reshape(blocks * slabs, slab_rows, chunk)
    cellwise = lax.all_to_all(updated, ("blk", "grid"), 0, 0, tiled=True)

    devices = blocks * slabs
    cell_count = NX * NY * NZ
    if devices * slab_rows <= 512 and devices % PANEL == 0 and chunk % LANES == 0:
        local = pl.pallas_call(
            gram_kernel,
            out_shape=jax.ShapeDtypeStruct((devices, devices * devices // LANES, LANES), F32),
            in_specs=[VMEM],
            out_specs=VMEM,
        )(cellwise)
        parts = lax.all_to_all(local, ("blk", "grid"), 0, 0, tiled=True)
        return pl.pallas_call(
            functools.partial(rotate_kernel, 1.0 / cell_count),
            out_shape=(
                jax.ShapeDtypeStruct(cellwise.shape, BF),
                jax.ShapeDtypeStruct((devices, devices), F32),
            ),
            in_specs=[VMEM, VMEM],
            out_specs=(VMEM, VMEM),
        )(parts, cellwise)
    flat = cellwise.reshape(devices, slab_rows * chunk)
    local = jnp.dot(flat, flat.T, preferred_element_type=F32)
    intersection = lax.psum(local, ("blk", "grid")) / cell_count
    factor = jnp.linalg.cholesky(intersection)
    identity = jnp.eye(devices, dtype=F32)
    inverse = jax.scipy.linalg.solve_triangular(factor, identity, lower=True).astype(BF)
    rotated = product(inverse, flat).astype(BF)
    return (rotated.reshape(cellwise.shape), intersection)


def solution(mesh):
    in_specs = (P("blk", "grid", None),)
    out_specs = (P(None, "grid", "blk"), P())
    return jax.shard_map(body, mesh=mesh, in_specs=in_specs, out_specs=out_specs, check_vma=False)
```

```python
import functools

import jax
import jax.numpy as jnp
from jax import lax
from jax.experimental import pallas as pl
from jax.experimental.pallas import tpu as pltpu
from jax.sharding import PartitionSpec as P


NX = 64
NY = 64
NZ = 64
STEPS = 2

exchange_fraction = 0.25
screening = 1.0

BF = jnp.bfloat16
F32 = jnp.float32
VMEM = pl.BlockSpec(memory_space=pltpu.VMEM)
SMEM = pl.BlockSpec(memory_space=pltpu.SMEM)
LANES = 128
ROW_PAD = 8
QUAD = 4
UNROLL = 4
PANEL = 8


def product(a, b):
    return jnp.dot(a, b, preferred_element_type=F32)


def sine_tables(rows, columns):
    angle = jnp.pi * (rows[:, :, None] + 1.0) * (columns[:, None, :] + 1.0) / (NX + 1)
    return (jnp.sqrt(2.0 / (NX + 1)) * jnp.sin(angle)).astype(BF)


def eigen_values(length):
    index = jnp.arange(length).astype(F32)
    return 2.0 - 2.0 * jnp.cos(jnp.pi * (index + 1.0) / (length + 1))


def table_kernel(sine_ref, lam_ref, lanes_ref, diag_ref, weight_ref):
    count, n, _ = sine_ref.shape
    size = diag_ref.shape[1]
    down = lax.broadcasted_iota(jnp.int32, (size, size), 0) // n
    along = lax.broadcasted_iota(jnp.int32, (size, size), 1) // n
    for i in range(count):
        table = sine_ref[i].astype(F32)
        table = jnp.concatenate([table] * (size // n), 1)
        table = jnp.concatenate([table] * (size // n), 0)
        diag_ref[i] = jnp.where(down == along, table, 0.0).astype(BF)
    columns = lam_ref[...]
    lanes = lanes_ref[...]
    for k in range(n):
        total = screening + columns[k:k + 1, :] + columns + lanes
        weight_ref[k * n:(k + 1) * n, :] = 1.0 / total


def make_tables(here):
    cells = jnp.arange(NX).astype(F32)
    here = here.astype(F32)
    sine = sine_tables(jnp.stack([cells, cells, here]), jnp.stack([cells, here, cells]))
    lam = eigen_values(NX)
    size = QUAD * NX
    return pl.pallas_call(
        table_kernel,
        out_shape=(
            jax.ShapeDtypeStruct((3, size, size), BF),
            jax.ShapeDtypeStruct((NX * NY, LANES), F32),
        ),
        in_specs=[VMEM] * 3,
        out_specs=(VMEM, VMEM),
        cost_estimate=pl.CostEstimate(flops=1 << 26, bytes_accessed=3 << 20, transcendentals=0),
    )(sine, jnp.broadcast_to(lam[:, None], (NX, LANES)),
      jnp.concatenate([lam] * (LANES // NZ))[None, :])


def block_kernel(slabs, parts, final, rest):
    own = rest[:slabs]
    src = [rest[slabs + p * slabs:slabs + (p + 1) * slabs] for p in range(parts)]
    rest = rest[slabs * (parts + 1):]
    pos_ref, tab_ref, w_ref = rest[:3]
    rest = rest[3:]
    if final:
        acc_ref, out_ref, grouped_ref, work_ref = rest
    else:
        out_ref, grouped_ref, work_ref = rest
    each = src[0][0].shape[0]
    count = each * parts
    rows = src[0][0].shape[1]
    halves = count * NZ // LANES
    width = QUAD * NZ
    pitch = work_ref.shape[1] // NY

    def tile(refs, lead, off, size):
        parts = [r[lead + (slice(None), pl.ds(off, size))] for r in refs]
        return jnp.concatenate(parts, 0)

    def load_rows(first):
        parts = []
        for q in range(QUAD):
            at = pl.multiple_of((first + q) * pitch, 8)
            parts.append(
                jnp.concatenate([work_ref[h, pl.ds(at, NX), :] for h in range(halves)], 1)
            )
        return jnp.concatenate(parts, 0)

    def forward(t, carry):
        off = pl.multiple_of(t * width, width)
        at = pl.multiple_of(t * QUAD * NX, QUAD * NX)
        mine = tile(own, (), off, width)
        others = [tile(src[j // each], (j % each,), off, width) for j in range(count)]
        pairs = [mine * other for other in others]
        cut = [slice(q * NZ, (q + 1) * NZ) for q in range(QUAD)]
        density = jnp.concatenate(
            [jnp.concatenate([p[:, c] for p in pairs], 1) for c in cut], 0)
        grouped_ref[pl.ds(at, QUAD * NX), :] = jnp.concatenate(
            [jnp.concatenate([o[:, c] for o in others], 1) for c in cut], 0)
        first = product(density, tab_ref[0]).astype(BF)
        modes = product(tab_ref[1], first)
        for q in range(QUAD):
            to = pl.multiple_of((t * QUAD + q) * pitch, 8)
            for h in range(halves):
                work_ref[h, pl.ds(to, NX), :] = modes[q * NX:(q + 1) * NX, h * LANES:(h + 1) * LANES]
        return carry

    def solve(t, carry):
        at = pl.multiple_of(t * QUAD * NY, QUAD * NY)
        modes = jnp.concatenate([
            jnp.concatenate(
                [work_ref[h, pl.ds(t * QUAD + q, NY, stride=pitch), :] for h in range(halves)], 1)
            for q in range(QUAD)], 0).astype(BF)
        weights = jnp.concatenate([w_ref[pl.ds(at, QUAD * NY), :]] * halves, 1)
        scaled = (product(tab_ref[0], modes) * weights).astype(BF)
        back = product(tab_ref[0], scaled)
        for q in range(QUAD):
            for h in range(halves):
                work_ref[h, pl.ds(t * QUAD + q, NY, stride=pitch), :] = (
                    back[q * NY:(q + 1) * NY, h * LANES:(h + 1) * LANES])
        return carry

    lane = lax.broadcasted_iota(jnp.int32, (NX, LANES), 1)
    per_tile = LANES // NZ

    def backward(t, carry):
        at = pl.multiple_of(t * QUAD * NX, QUAD * NX)
        third = product(tab_ref[2], load_rows(t * QUAD).astype(BF)).astype(BF)
        potential = product(third, tab_ref[0])
        terms = potential * grouped_ref[pl.ds(at, QUAD * NX), :].astype(F32)
        total = terms[:, :LANES]
        for h in range(1, halves):
            total = total + terms[:, h * LANES:(h + 1) * LANES]
        total = total + pltpu.roll(total, NZ, 1)
        for q in range(0, QUAD, per_tile):
            exchange = jnp.where(
                lane < NZ, total[q * NX:(q + 1) * NX], total[(q + 1) * NX:(q + 2) * NX])
            off = pl.multiple_of((t * QUAD + q) * NZ, LANES)
            if not final:
                out_ref[:, pl.ds(off, LANES)] = exchange
                continue
            exchange = exchange + acc_ref[:, pl.ds(off, LANES)]
            mine = tile(own, (), off, LANES).astype(F32)
            updated = (mine - exchange_fraction * exchange).astype(BF)
            for r in range(slabs):
                part = updated[r * rows:(r + 1) * rows]
                if len(out_ref.shape) == 4:
                    share = out_ref.shape[3] // LANES
                    index = (t * QUAD + q) * NZ // LANES
                    to = pl.multiple_of((index % share) * LANES, LANES)
                    out_ref[index // share, pos_ref[r], :, pl.ds(to, LANES)] = part
                else:
                    out_ref[pos_ref[r], :, pl.ds(off, LANES)] = part
        return carry

    lax.fori_loop(0, NY // QUAD, forward, 0, unroll=UNROLL)
    lax.fori_loop(0, NX // QUAD, solve, 0, unroll=UNROLL)
    lax.fori_loop(0, NY // QUAD, backward, 0, unroll=UNROLL)


def add_block(own, src, tables, acc, out_shape):
    slabs = len(own)
    count = sum(part[0].shape[0] for part in src)
    final = acc is not None
    lead = () if acc is None else (acc,)
    flops = 12 * count * NX * NY * NZ * NZ * 4
    return pl.pallas_call(
        lambda *refs: block_kernel(slabs, len(src), final, refs),
        out_shape=out_shape,
        in_specs=[VMEM] * ((1 + len(src)) * slabs) + [SMEM] + [VMEM] * (2 + len(lead)),
        out_specs=VMEM,
        scratch_shapes=[
            pltpu.VMEM((NY * NX, count * NZ), BF),
            pltpu.VMEM((count * NZ // LANES, NY * (NX + ROW_PAD), LANES), F32),
        ],
        compiler_params=pltpu.CompilerParams(vmem_limit_bytes=40 * 1024 * 1024),
        cost_estimate=pl.CostEstimate(flops=flops, bytes_accessed=8 << 20, transcendentals=0),
    )(*own, *[slab for part in src for slab in part], *tables, *lead)


def gram_kernel(x_ref, out_ref):
    orbs, rows, lanes = x_ref.shape
    flat = x_ref[...].reshape(orbs * rows, lanes)
    full = lax.dot_general(flat, flat, (((1,), (1,)), ((), ())), preferred_element_type=F32)
    down = lax.broadcasted_iota(jnp.int32, (rows, orbs * rows), 0)
    along = lax.broadcasted_iota(jnp.int32, (rows, orbs * rows), 1)
    same = down == along % rows
    half = [
        jnp.sum(jnp.where(same, full[o * rows:(o + 1) * rows], 0.0), axis=0, keepdims=True)
        for o in range(orbs)
    ]
    half = jnp.concatenate(half, 0)
    gram = jnp.sum(half.T.reshape(orbs, rows, orbs), axis=1)
    deep = orbs * orbs // LANES
    packed = jnp.concatenate([gram[q * deep:(q + 1) * deep] for q in range(orbs // deep)], 1)
    out_ref[...] = jnp.broadcast_to(packed[None], out_ref.shape)


def rotate_kernel(scale, parts_ref, x_ref, out_ref, gram_ref):
    orbs, rows, lanes = x_ref.shape
    packed = jnp.sum(parts_ref[...], axis=0) * scale
    gram = jnp.concatenate(
        [packed[:, q * orbs:(q + 1) * orbs] for q in range(LANES // orbs)], 0)
    gram_ref[...] = gram
    down = lax.broadcasted_iota(jnp.int32, (orbs, orbs), 0)
    along = lax.broadcasted_iota(jnp.int32, (orbs, orbs), 1)
    eye = jnp.where(down == along, 1.0, 0.0)
    zero = jnp.zeros((orbs, LANES - 2 * orbs), F32)
    work = jnp.concatenate([gram, eye, zero], 1)
    row = lax.broadcasted_iota(jnp.int32, (orbs, LANES), 0)
    pivots = jnp.zeros((orbs, LANES), F32)
    for first in range(0, orbs, PANEL):
        columns = [
            jnp.broadcast_to(work[:, c:c + 1], (orbs, LANES)) for c in range(first, first + PANEL)
        ]
        for k in range(first, first + PANEL):
            column = columns[k - first]
            pivot = column[k:k + 1, :]
            pivots = jnp.where(row == k, pivot, pivots)
            factor = jnp.where(row > k, column * (1.0 / pivot), 0.0)
            work = work - factor * work[k:k + 1, :]
            for c in range(k - first + 1, PANEL):
                columns[c] = columns[c] - factor * columns[c][k:k + 1, :]
    work = work * (1.0 / jnp.sqrt(pivots))
    inverse = work[:, orbs:2 * orbs].astype(BF)
    tall = lax.broadcasted_iota(jnp.int32, (orbs * rows, orbs), 0) // rows
    wide = lax.broadcasted_iota(jnp.int32, (orbs * rows, orbs), 1)
    pick = jnp.where(tall == wide, 1.0, 0.0).astype(BF)
    spread = product(pick, inverse).astype(BF)
    spread = lax.dot_general(spread, pick, (((1,), (1,)), ((), ())), preferred_element_type=F32)
    i = lax.broadcasted_iota(jnp.int32, (orbs * rows, 1), 0) % rows
    j = lax.broadcasted_iota(jnp.int32, (1, orbs * rows), 1) % rows
    spread = jnp.where(i == j, spread, 0.0).astype(BF)
    flat = x_ref[...].reshape(orbs * rows, lanes)
    out_ref[...] = product(spread, flat).astype(BF).reshape(orbs, rows, lanes)


def exchanged(x, axis, by):
    return lax.ppermute(x, axis, [(i, i ^ by) for i in range(lax.axis_size(axis))])


def completed(slab, other):
    top = lax.axis_size("grid") // 2
    slabs = {0: slab, top: other}
    bit = top // 2
    while bit:
        for r in list(slabs):
            slabs[r | bit] = exchanged(slabs[r], "grid", bit)
        bit //= 2
    return [slabs[r] for r in range(2 * top)]


def body(orbitals):
    orb_count, slab_rows, plane_cells = orbitals.shape
    slabs = lax.axis_size("grid")
    blocks = lax.axis_size("blk")
    assert orb_count == slabs and slab_rows * slabs == NX and blocks % 2 == 0 and STEPS == 2
    grid_index = lax.axis_index("grid")
    order = jnp.arange(slabs) ^ grid_index

    here = (order[:, None] * slab_rows + jnp.arange(slab_rows)[None, :]).reshape(NX)
    diagonals, weights = make_tables(here)

    top = slabs // 2
    half = orb_count // 2
    even = lax.axis_index("blk") % 2 == 0

    def shifted(x):
        return lax.ppermute(x, "blk", [(i, (i + 2) % blocks) for i in range(blocks)])

    def relayed(mine, received):
        return exchanged(jnp.where(even, mine, received), "blk", 1)

    mine = lax.optimization_barrier([orbitals[:half], orbitals[half:]])
    far = [shifted(mine[i]) for i in range(2)]
    across = exchanged(orbitals, "grid", top)
    across_half = lax.optimization_barrier(across[:half])
    first, diagonals, weights = lax.optimization_barrier((far[0], diagonals, weights))
    tables = (order.astype(jnp.int32), diagonals, weights)
    near = [relayed(mine[0], first), relayed(mine[1], far[1])]
    far_other = [shifted(across_half), exchanged(far[1], "grid", top)]
    near_other = [relayed(across_half, far_other[0]), exchanged(near[1], "grid", top)]

    own = {}
    for r in range(top):
        for held, block in ((0, orbitals), (top, across)):
            piece = lax.dynamic_index_in_dim(block, grid_index ^ r, 0, keepdims=False)
            own[r | held] = exchanged(piece, "grid", r) if r else piece
    own = [own[r] for r in range(slabs)]

    far = [completed(far[i], far_other[i]) for i in range(2)]
    acc = add_block(own, far, tables, None, jax.ShapeDtypeStruct((NX, plane_cells), F32))
    near_other, acc = lax.optimization_barrier((near_other, acc))
    near = [completed(near[i], near_other[i]) for i in range(2)]
    chunk = plane_cells // blocks
    if chunk % LANES == 0:
        shape = (blocks, slabs, slab_rows, chunk)
    else:
        shape = (slabs, slab_rows, plane_cells)
    updated = add_block(own, near, tables, acc, jax.ShapeDtypeStruct(shape, BF))
    if chunk % LANES:
        updated = updated.reshape(slabs, slab_rows, blocks, chunk).transpose(2, 0, 1, 3)
    updated = updated.reshape(blocks * slabs, slab_rows, chunk)
    cellwise = lax.all_to_all(updated, ("blk", "grid"), 0, 0, tiled=True)

    devices = blocks * slabs
    cell_count = NX * NY * NZ
    if devices * slab_rows <= 512 and devices % PANEL == 0 and chunk % LANES == 0:
        local = pl.pallas_call(
            gram_kernel,
            out_shape=jax.ShapeDtypeStruct((devices, devices * devices // LANES, LANES), F32),
            in_specs=[VMEM],
            out_specs=VMEM,
        )(cellwise)
        parts = lax.all_to_all(local, ("blk", "grid"), 0, 0, tiled=True)
        return pl.pallas_call(
            functools.partial(rotate_kernel, 1.0 / cell_count),
            out_shape=(
                jax.ShapeDtypeStruct(cellwise.shape, BF),
                jax.ShapeDtypeStruct((devices, devices), F32),
            ),
            in_specs=[VMEM, VMEM],
            out_specs=(VMEM, VMEM),
        )(parts, cellwise)
    flat = cellwise.reshape(devices, slab_rows * chunk)
    local = jnp.dot(flat, flat.T, preferred_element_type=F32)
    intersection = lax.psum(local, ("blk", "grid")) / cell_count
    factor = jnp.linalg.cholesky(intersection)
    identity = jnp.eye(devices, dtype=F32)
    inverse = jax.scipy.linalg.solve_triangular(factor, identity, lower=True).astype(BF)
    rotated = product(inverse, flat).astype(BF)
    return (rotated.reshape(cellwise.shape), intersection)


def solution(mesh):
    in_specs = (P("blk", "grid", None),)
    out_specs = (P(None, "grid", "blk"), P())
    return jax.shard_map(body, mesh=mesh, in_specs=in_specs, out_specs=out_specs, check_vma=False)
```

```python
import functools

import jax
import jax.numpy as jnp
from jax import lax
from jax.experimental import pallas as pl
from jax.experimental.pallas import tpu as pltpu
from jax.sharding import PartitionSpec as P


NX = 64
NY = 64
NZ = 64
STEPS = 2

exchange_fraction = 0.25
screening = 1.0

BF = jnp.bfloat16
F32 = jnp.float32
VMEM = pl.BlockSpec(memory_space=pltpu.VMEM)
SMEM = pl.BlockSpec(memory_space=pltpu.SMEM)
LANES = 128
ROW_PAD = 1
QUAD = 4
PANEL = 8


def product(a, b):
    return jnp.dot(a, b, preferred_element_type=F32)


def sines(rows, columns, length):
    angle = jnp.pi * (rows + 1.0) * (columns + 1.0) / (length + 1)
    return jnp.sqrt(2.0 / (length + 1)) * jnp.sin(angle)


def eigen_values(index, length):
    return 2.0 - 2.0 * jnp.cos(jnp.pi * (index + 1.0) / (length + 1))


def table_kernel(slab_rows, order_ref, diag_ref, weight_ref):
    size = diag_ref.shape[1]
    copies = size // NX

    def cells_of(position):
        slab = position // slab_rows
        start = jnp.zeros_like(position)
        for r in range(NX // slab_rows):
            start = jnp.where(slab == r, order_ref[r] * slab_rows, start)
        return start + position % slab_rows

    shape = (NX, LANES)
    down = lax.broadcasted_iota(jnp.int32, shape, 0)
    along = lax.broadcasted_iota(jnp.int32, shape, 1) % NX
    pairs = (
        (down, along),
        (down, cells_of(along)),
        (cells_of(down), along),
    )
    same = (
        lax.broadcasted_iota(jnp.int32, (NX, size), 1) // NX
    )
    for i, (row, column) in enumerate(pairs):
        table = sines(row.astype(F32), column.astype(F32), NX)
        table = jnp.concatenate([table] * (size // LANES), 1)
        for c in range(copies):
            diag_ref[i, c * NX:(c + 1) * NX, :] = jnp.where(same == c, table, 0.0).astype(BF)
    lam = eigen_values(down.astype(F32), NX)
    plane = screening + lam + eigen_values(along.astype(F32), NZ)
    for k in range(NX):
        weight_ref[k * NY:(k + 1) * NY, :] = 1.0 / (lam[k:k + 1, :] + plane)


def make_tables(order, slab_rows):
    size = QUAD * NX
    return pl.pallas_call(
        functools.partial(table_kernel, slab_rows),
        out_shape=(
            jax.ShapeDtypeStruct((3, size, size), BF),
            jax.ShapeDtypeStruct((NX * NY, LANES), F32),
        ),
        in_specs=[SMEM],
        out_specs=(VMEM, VMEM),
        cost_estimate=pl.CostEstimate(flops=1 << 28, bytes_accessed=3 << 20, transcendentals=0),
    )(order)


def block_kernel(slabs, parts, final, rest):
    own = rest[:slabs]
    src = [rest[slabs + p * slabs:slabs + (p + 1) * slabs] for p in range(parts)]
    rest = rest[slabs * (parts + 1):]
    pos_ref, tab_ref, w_ref = rest[:3]
    rest = rest[3:]
    if final:
        acc_ref, out_ref, grouped_ref, work_ref = rest
    else:
        out_ref, grouped_ref, work_ref = rest
    each = src[0][0].shape[0]
    count = each * parts
    rows = src[0][0].shape[1]
    halves = count * NZ // LANES
    width = QUAD * NZ
    pitch = work_ref.shape[1] // NY

    def tile(refs, lead, off, size):
        parts = [r[lead + (slice(None), pl.ds(off, size))] for r in refs]
        return jnp.concatenate(parts, 0)

    def load_rows(first):
        parts = []
        for q in range(QUAD):
            at = (first + q) * pitch
            parts.append(
                jnp.concatenate([work_ref[h, pl.ds(at, NX), :] for h in range(halves)], 1)
            )
        return jnp.concatenate(parts, 0)

    def forward(t):
        off = t * width
        at = t * QUAD * NX
        mine = tile(own, (), off, width)
        others = [tile(src[j // each], (j % each,), off, width) for j in range(count)]
        pairs = [mine * other for other in others]
        cut = [slice(q * NZ, (q + 1) * NZ) for q in range(QUAD)]
        density = jnp.concatenate(
            [jnp.concatenate([p[:, c] for p in pairs], 1) for c in cut], 0)
        grouped_ref[pl.ds(at, QUAD * NX), :] = jnp.concatenate(
            [jnp.concatenate([o[:, c] for o in others], 1) for c in cut], 0)
        first = product(density, tab_ref[0]).astype(BF)
        modes = product(tab_ref[1], first)
        for q in range(QUAD):
            to = (t * QUAD + q) * pitch
            for h in range(halves):
                work_ref[h, pl.ds(to, NX), :] = modes[q * NX:(q + 1) * NX, h * LANES:(h + 1) * LANES]

    def solve(t):
        at = t * QUAD * NY
        modes = jnp.concatenate([
            jnp.concatenate(
                [work_ref[h, pl.ds(t * QUAD + q, NY, stride=pitch), :] for h in range(halves)], 1)
            for q in range(QUAD)], 0).astype(BF)
        weights = jnp.concatenate([w_ref[pl.ds(at, QUAD * NY), :]] * halves, 1)
        scaled = (product(tab_ref[0], modes) * weights).astype(BF)
        back = product(tab_ref[0], scaled)
        for q in range(QUAD):
            for h in range(halves):
                work_ref[h, pl.ds(t * QUAD + q, NY, stride=pitch), :] = (
                    back[q * NY:(q + 1) * NY, h * LANES:(h + 1) * LANES])

    lane = lax.broadcasted_iota(jnp.int32, (NX, LANES), 1)
    per_tile = LANES // NZ

    def backward(t):
        at = t * QUAD * NX
        third = product(tab_ref[2], load_rows(t * QUAD).astype(BF)).astype(BF)
        potential = product(third, tab_ref[0])
        terms = potential * grouped_ref[pl.ds(at, QUAD * NX), :].astype(F32)
        total = terms[:, :LANES]
        for h in range(1, halves):
            total = total + terms[:, h * LANES:(h + 1) * LANES]
        total = total + pltpu.roll(total, NZ, 1)
        for q in range(0, QUAD, per_tile):
            exchange = jnp.where(
                lane < NZ, total[q * NX:(q + 1) * NX], total[(q + 1) * NX:(q + 2) * NX])
            off = (t * QUAD + q) * NZ
            if not final:
                out_ref[:, pl.ds(off, LANES)] = exchange
                continue
            exchange = exchange + acc_ref[:, pl.ds(off, LANES)]
            mine = tile(own, (), off, LANES).astype(F32)
            updated = (mine - exchange_fraction * exchange).astype(BF)
            for r in range(slabs):
                part = updated[r * rows:(r + 1) * rows]
                if len(out_ref.shape) == 4:
                    share = out_ref.shape[3] // LANES
                    index = (t * QUAD + q) * NZ // LANES
                    to = (index % share) * LANES
                    out_ref[index // share, pos_ref[r], :, pl.ds(to, LANES)] = part
                else:
                    out_ref[pos_ref[r], :, pl.ds(off, LANES)] = part

    for step, trips in ((forward, NY // QUAD), (solve, NX // QUAD), (backward, NY // QUAD)):
        for t in range(trips):
            step(t)


def add_block(own, src, tables, acc, out_shape):
    slabs = len(own)
    count = sum(part[0].shape[0] for part in src)
    final = acc is not None
    lead = () if acc is None else (acc,)
    flops = 12 * count * NX * NY * NZ * NZ * 4
    return pl.pallas_call(
        lambda *refs: block_kernel(slabs, len(src), final, refs),
        out_shape=out_shape,
        in_specs=[VMEM] * ((1 + len(src)) * slabs) + [SMEM] + [VMEM] * (2 + len(lead)),
        out_specs=VMEM,
        scratch_shapes=[
            pltpu.VMEM((NY * NX, count * NZ), BF),
            pltpu.VMEM((count * NZ // LANES, NY * (NX + ROW_PAD), LANES), F32),
        ],
        compiler_params=pltpu.CompilerParams(vmem_limit_bytes=40 * 1024 * 1024),
        cost_estimate=pl.CostEstimate(flops=flops, bytes_accessed=8 << 20, transcendentals=0),
    )(*own, *[slab for part in src for slab in part], *tables, *lead)


def gram_kernel(x_ref, out_ref):
    orbs, rows, lanes = x_ref.shape
    flat = x_ref[...].reshape(orbs * rows, lanes)
    full = lax.dot_general(flat, flat, (((1,), (1,)), ((), ())), preferred_element_type=F32)
    down = lax.broadcasted_iota(jnp.int32, (rows, orbs * rows), 0)
    along = lax.broadcasted_iota(jnp.int32, (rows, orbs * rows), 1)
    same = down == along % rows
    half = [
        jnp.sum(jnp.where(same, full[o * rows:(o + 1) * rows], 0.0), axis=0, keepdims=True)
        for o in range(orbs)
    ]
    half = jnp.concatenate(half, 0)
    gram = jnp.sum(half.T.reshape(orbs, rows, orbs), axis=1)
    deep = orbs * orbs // LANES
    packed = jnp.concatenate([gram[q * deep:(q + 1) * deep] for q in range(orbs // deep)], 1)
    out_ref[...] = jnp.broadcast_to(packed[None], out_ref.shape)


def rotate_kernel(scale, parts_ref, x_ref, out_ref, gram_ref):
    orbs, rows, lanes = x_ref.shape
    packed = jnp.sum(parts_ref[...], axis=0) * scale
    gram = jnp.concatenate(
        [packed[:, q * orbs:(q + 1) * orbs] for q in range(LANES // orbs)], 0)
    gram_ref[...] = gram
    down = lax.broadcasted_iota(jnp.int32, (orbs, orbs), 0)
    along = lax.broadcasted_iota(jnp.int32, (orbs, orbs), 1)
    eye = jnp.where(down == along, 1.0, 0.0)
    zero = jnp.zeros((orbs, LANES - 2 * orbs), F32)
    work = jnp.concatenate([gram, eye, zero], 1)
    row = lax.broadcasted_iota(jnp.int32, (orbs, LANES), 0)
    pivots = jnp.zeros((orbs, LANES), F32)
    for first in range(0, orbs, PANEL):
        columns = [
            jnp.broadcast_to(work[:, c:c + 1], (orbs, LANES)) for c in range(first, first + PANEL)
        ]
        for k in range(first, first + PANEL):
            column = columns[k - first]
            pivot = column[k:k + 1, :]
            pivots = jnp.where(row == k, pivot, pivots)
            factor = jnp.where(row > k, column * (1.0 / pivot), 0.0)
            work = work - factor * work[k:k + 1, :]
            for c in range(k - first + 1, PANEL):
                columns[c] = columns[c] - factor * columns[c][k:k + 1, :]
    work = work * (1.0 / jnp.sqrt(pivots))
    inverse = work[:, orbs:2 * orbs].astype(BF)
    tall = lax.broadcasted_iota(jnp.int32, (orbs * rows, orbs), 0) // rows
    wide = lax.broadcasted_iota(jnp.int32, (orbs * rows, orbs), 1)
    pick = jnp.where(tall == wide, 1.0, 0.0).astype(BF)
    spread = product(pick, inverse).astype(BF)
    spread = lax.dot_general(spread, pick, (((1,), (1,)), ((), ())), preferred_element_type=F32)
    i = lax.broadcasted_iota(jnp.int32, (orbs * rows, 1), 0) % rows
    j = lax.broadcasted_iota(jnp.int32, (1, orbs * rows), 1) % rows
    spread = jnp.where(i == j, spread, 0.0).astype(BF)
    flat = x_ref[...].reshape(orbs * rows, lanes)
    out_ref[...] = product(spread, flat).astype(BF).reshape(orbs, rows, lanes)


def exchanged(x, axis, by):
    return lax.ppermute(x, axis, [(i, i ^ by) for i in range(lax.axis_size(axis))])


def completed(slab, other):
    top = lax.axis_size("grid") // 2
    slabs = {0: slab, top: other}
    bit = top // 2
    while bit:
        for r in list(slabs):
            slabs[r | bit] = exchanged(slabs[r], "grid", bit)
        bit //= 2
    return [slabs[r] for r in range(2 * top)]


def body(orbitals):
    orb_count, slab_rows, plane_cells = orbitals.shape
    slabs = lax.axis_size("grid")
    blocks = lax.axis_size("blk")
    assert orb_count == slabs and slab_rows * slabs == NX and blocks % 2 == 0 and STEPS == 2
    grid_index = lax.axis_index("grid")
    order = (jnp.arange(slabs) ^ grid_index).astype(jnp.int32)

    diagonals, weights = make_tables(order, slab_rows)
    top = slabs // 2
    half = orb_count // 2
    even = lax.axis_index("blk") % 2 == 0

    def shifted(x):
        return lax.ppermute(x, "blk", [(i, (i + 2) % blocks) for i in range(blocks)])

    def relayed(mine, received):
        return exchanged(jnp.where(even, mine, received), "blk", 1)

    mine = lax.optimization_barrier([orbitals[:half], orbitals[half:]])
    far = [shifted(mine[i]) for i in range(2)]
    across = exchanged(orbitals, "grid", top)
    across_half = lax.optimization_barrier(across[:half])
    near = [relayed(mine[i], far[i]) for i in range(2)]
    far_other = [shifted(across_half), exchanged(far[1], "grid", top)]
    across_half, diagonals, weights = lax.optimization_barrier(
        (across_half, diagonals, weights))
    tables = (order, diagonals, weights)
    near_other = [relayed(across_half, far_other[0]), exchanged(near[1], "grid", top)]

    own = {}
    for r in range(top):
        for held, block in ((0, orbitals), (top, across)):
            piece = lax.dynamic_index_in_dim(block, grid_index ^ r, 0, keepdims=False)
            own[r | held] = exchanged(piece, "grid", r) if r else piece
    own = [own[r] for r in range(slabs)]

    far = [completed(far[i], far_other[i]) for i in range(2)]
    acc = add_block(own, far, tables, None, jax.ShapeDtypeStruct((NX, plane_cells), F32))
    near_other, acc = lax.optimization_barrier((near_other, acc))
    near = [completed(near[i], near_other[i]) for i in range(2)]
    chunk = plane_cells // blocks
    if chunk % LANES == 0:
        shape = (blocks, slabs, slab_rows, chunk)
    else:
        shape = (slabs, slab_rows, plane_cells)
    updated = add_block(own, near, tables, acc, jax.ShapeDtypeStruct(shape, BF))
    if chunk % LANES:
        updated = updated.reshape(slabs, slab_rows, blocks, chunk).transpose(2, 0, 1, 3)
    updated = updated.reshape(blocks * slabs, slab_rows, chunk)
    cellwise = lax.all_to_all(updated, ("blk", "grid"), 0, 0, tiled=True)

    devices = blocks * slabs
    cell_count = NX * NY * NZ
    if devices * slab_rows <= 512 and devices % PANEL == 0 and chunk % LANES == 0:
        local = pl.pallas_call(
            gram_kernel,
            out_shape=jax.ShapeDtypeStruct((devices, devices * devices // LANES, LANES), F32),
            in_specs=[VMEM],
            out_specs=VMEM,
        )(cellwise)
        parts = lax.all_to_all(local, ("blk", "grid"), 0, 0, tiled=True)
        return pl.pallas_call(
            functools.partial(rotate_kernel, 1.0 / cell_count),
            out_shape=(
                jax.ShapeDtypeStruct(cellwise.shape, BF),
                jax.ShapeDtypeStruct((devices, devices), F32),
            ),
            in_specs=[VMEM, VMEM],
            out_specs=(VMEM, VMEM),
        )(parts, cellwise)
    flat = cellwise.reshape(devices, slab_rows * chunk)
    local = jnp.dot(flat, flat.T, preferred_element_type=F32)
    intersection = lax.psum(local, ("blk", "grid")) / cell_count
    factor = jnp.linalg.cholesky(intersection)
    identity = jnp.eye(devices, dtype=F32)
    inverse = jax.scipy.linalg.solve_triangular(factor, identity, lower=True).astype(BF)
    rotated = product(inverse, flat).astype(BF)
    return (rotated.reshape(cellwise.shape), intersection)


def solution(mesh):
    in_specs = (P("blk", "grid", None),)
    out_specs = (P(None, "grid", "blk"), P())
    return jax.shard_map(body, mesh=mesh, in_specs=in_specs, out_specs=out_specs, check_vma=False)
```

```python
import functools

import jax
import jax.numpy as jnp
from jax import lax
from jax.experimental import pallas as pl
from jax.experimental.pallas import tpu as pltpu
from jax.sharding import PartitionSpec as P


NX = 64
NY = 64
NZ = 64
STEPS = 2

exchange_fraction = 0.25
screening = 1.0

BF = jnp.bfloat16
F32 = jnp.float32
VMEM = pl.BlockSpec(memory_space=pltpu.VMEM)
SMEM = pl.BlockSpec(memory_space=pltpu.SMEM)
LANES = 128
ROW_PAD = 1
QUAD = 4
PANEL = 8


def product(a, b):
    return jnp.dot(a, b, preferred_element_type=F32)


def sines(rows, columns, length):
    angle = jnp.pi * (rows + 1.0) * (columns + 1.0) / (length + 1)
    return jnp.sqrt(2.0 / (length + 1)) * jnp.sin(angle)


def eigen_values(index, length):
    return 2.0 - 2.0 * jnp.cos(jnp.pi * (index + 1.0) / (length + 1))


def table_kernel(slab_rows, diag_ref, weight_ref):
    size = diag_ref.shape[1]
    copies = size // NX
    grid_index = lax.axis_index("grid")

    def cells_of(position):
        slab = position // slab_rows
        start = jnp.zeros_like(position)
        for r in range(NX // slab_rows):
            start = jnp.where(slab == r, (grid_index ^ r) * slab_rows, start)
        return start + position % slab_rows

    shape = (NX, LANES)
    down = lax.broadcasted_iota(jnp.int32, shape, 0)
    along = lax.broadcasted_iota(jnp.int32, shape, 1) % NX
    pairs = (
        (down, along),
        (down, cells_of(along)),
        (cells_of(down), along),
    )
    same = (
        lax.broadcasted_iota(jnp.int32, (NX, size), 1) // NX
    )
    for i, (row, column) in enumerate(pairs):
        table = sines(row.astype(F32), column.astype(F32), NX)
        table = jnp.concatenate([table] * (size // LANES), 1)
        for c in range(copies):
            diag_ref[i, c * NX:(c + 1) * NX, :] = jnp.where(same == c, table, 0.0).astype(BF)
    lam = eigen_values(down.astype(F32), NX)
    plane = screening + lam + eigen_values(along.astype(F32), NZ)
    for k in range(NX):
        weight_ref[k * NY:(k + 1) * NY, :] = 1.0 / (lam[k:k + 1, :] + plane)


def make_tables(slab_rows):
    size = QUAD * NX
    return pl.pallas_call(
        functools.partial(table_kernel, slab_rows),
        out_shape=(
            jax.ShapeDtypeStruct((3, size, size), BF),
            jax.ShapeDtypeStruct((NX * NY, LANES), F32),
        ),
        out_specs=(VMEM, VMEM),
        cost_estimate=pl.CostEstimate(flops=1 << 28, bytes_accessed=3 << 20, transcendentals=0),
    )()


def block_kernel(slabs, final, rest):
    grid_index = lax.axis_index("grid")
    core, chip = grid_index % 2, grid_index // 2
    local = rest[:slabs]
    passed = rest[slabs:2 * slabs]
    src = rest[2 * slabs:3 * slabs]
    tab_ref, w_ref = rest[3 * slabs:3 * slabs + 2]
    rest = rest[3 * slabs + 2:]
    if final:
        acc_ref, keep_ref, send_ref, grouped_ref, work_ref = rest
    else:
        out_ref, grouped_ref, work_ref = rest
    owns = local[0].shape[0]
    count = src[0].shape[0]
    halves = owns * count * NZ // LANES
    width = QUAD * NZ
    pitch = work_ref.shape[1] // NY

    def tile(refs, j, off, size):
        return jnp.concatenate([r[j, :, pl.ds(off, size)] for r in refs], 0)

    def own_tile(o, off, size):
        return jnp.where(core == chip, tile(local, o, off, size), tile(passed, o, off, size))

    def forward(t):
        off = t * width
        at = t * QUAD * NX
        mine = [own_tile(o, off, width) for o in range(owns)]
        others = [tile(src, j, off, width) for j in range(count)]
        pairs = [m * other for m in mine for other in others]
        cut = [slice(q * NZ, (q + 1) * NZ) for q in range(QUAD)]
        density = jnp.concatenate(
            [jnp.concatenate([p[:, c] for p in pairs], 1) for c in cut], 0)
        grouped_ref[pl.ds(at, QUAD * NX), :] = jnp.concatenate(
            [jnp.concatenate([o[:, c] for o in others], 1) for c in cut], 0)
        first = product(density, tab_ref[0]).astype(BF)
        modes = product(tab_ref[1], first)
        for q in range(QUAD):
            to = (t * QUAD + q) * pitch
            for h in range(halves):
                work_ref[h, pl.ds(to, NX), :] = modes[q * NX:(q + 1) * NX, h * LANES:(h + 1) * LANES]

    def solve(t):
        at = t * QUAD * NY
        modes = jnp.concatenate([
            jnp.concatenate(
                [work_ref[h, pl.ds(t * QUAD + q, NY, stride=pitch), :] for h in range(halves)], 1)
            for q in range(QUAD)], 0).astype(BF)
        weights = jnp.concatenate([w_ref[pl.ds(at, QUAD * NY), :]] * halves, 1)
        scaled = (product(tab_ref[0], modes) * weights).astype(BF)
        back = product(tab_ref[0], scaled)
        for q in range(QUAD):
            for h in range(halves):
                work_ref[h, pl.ds(t * QUAD + q, NY, stride=pitch), :] = (
                    back[q * NY:(q + 1) * NY, h * LANES:(h + 1) * LANES])

    lane = lax.broadcasted_iota(jnp.int32, (NX, LANES), 1)

    def backward(t):
        at = t * QUAD * NX
        modes = jnp.concatenate([
            jnp.concatenate(
                [work_ref[h, pl.ds((t * QUAD + q) * pitch, NX), :] for h in range(halves)], 1)
            for q in range(QUAD)], 0).astype(BF)
        third = product(tab_ref[2], modes).astype(BF)
        potential = product(third, tab_ref[0])
        factor = grouped_ref[pl.ds(at, QUAD * NX), :].astype(F32)
        totals = []
        for o in range(owns):
            terms = potential[:, o * LANES:(o + 1) * LANES] * factor
            totals.append(terms + pltpu.roll(terms, NZ, 1))
        for q in range(0, QUAD, LANES // NZ):
            off = (t * QUAD + q) * NZ
            exchange = [
                jnp.where(lane < NZ, x[q * NX:(q + 1) * NX], x[(q + 1) * NX:(q + 2) * NX])
                for x in totals
            ]
            if not final:
                for o in range(owns):
                    out_ref[o, :, pl.ds(off, LANES)] = exchange[o]
                continue
            exchange = [
                exchange_fraction * (x + acc_ref[o, :, pl.ds(off, LANES)])
                for o, x in enumerate(exchange)
            ]
            own = [own_tile(o, off, LANES) for o in range(owns)]
            first = core == 0
            own = jnp.where(first, own[0], own[1]).astype(F32)
            keep_ref[:, pl.ds(off, LANES)] = own - jnp.where(first, exchange[0], exchange[1])
            send_ref[:, pl.ds(off, LANES)] = (
                jnp.where(first, exchange[1], exchange[0]).astype(send_ref.dtype))

    for step, trips in ((forward, NY // QUAD), (solve, NX // QUAD), (backward, NY // QUAD)):
        for t in range(trips):
            step(t)


def add_block(local, passed, src, tables, acc):
    slabs = len(local)
    owns, _, cells = local[0].shape
    count = src[0].shape[0]
    assert count * NZ == LANES and owns == 2
    final = acc is not None
    lead = () if acc is None else (acc,)
    flops = 12 * owns * count * NX * NY * NZ * NZ * 4
    if final:
        out_shape = (
            jax.ShapeDtypeStruct((NX, cells), F32), jax.ShapeDtypeStruct((NX, cells), BF))
    else:
        out_shape = jax.ShapeDtypeStruct((owns, NX, cells), F32)
    return pl.pallas_call(
        lambda *refs: block_kernel(slabs, final, refs),
        out_shape=out_shape,
        in_specs=[VMEM] * (3 * slabs + 2 + len(lead)),
        out_specs=(VMEM, VMEM) if final else VMEM,
        scratch_shapes=[
            pltpu.VMEM((NY * NX, count * NZ), BF),
            pltpu.VMEM((owns * count * NZ // LANES, NY * (NX + ROW_PAD), LANES), F32),
        ],
        compiler_params=pltpu.CompilerParams(vmem_limit_bytes=24 * 1024 * 1024),
        cost_estimate=pl.CostEstimate(flops=flops, bytes_accessed=8 << 20, transcendentals=0),
    )(*local, *passed, *src, *tables, *lead)


def combine_kernel(slabs, keep_ref, part_ref, out_ref):
    grid_index = lax.axis_index("grid")
    rows = keep_ref.shape[0] // slabs
    for r in range(slabs):
        other = (r ^ 1) * rows
        updated = keep_ref[r * rows:(r + 1) * rows] - part_ref[other:other + rows].astype(F32)
        updated = updated.astype(BF)
        if len(out_ref.shape) == 3:
            out_ref[grid_index ^ r] = updated
            continue
        share = out_ref.shape[3]
        for b in range(out_ref.shape[0]):
            out_ref[b, grid_index ^ r] = updated[:, b * share:(b + 1) * share]


def gram_kernel(x_ref, out_ref):
    orbs, rows, lanes = x_ref.shape
    flat = x_ref[...].reshape(orbs * rows, lanes)
    full = lax.dot_general(flat, flat, (((1,), (1,)), ((), ())), preferred_element_type=F32)
    down = lax.broadcasted_iota(jnp.int32, (rows, orbs * rows), 0)
    along = lax.broadcasted_iota(jnp.int32, (rows, orbs * rows), 1)
    same = down == along % rows
    half = [
        jnp.sum(jnp.where(same, full[o * rows:(o + 1) * rows], 0.0), axis=0, keepdims=True)
        for o in range(orbs)
    ]
    half = jnp.concatenate(half, 0)
    gram = jnp.sum(half.T.reshape(orbs, rows, orbs), axis=1)
    deep = orbs * orbs // LANES
    packed = jnp.concatenate([gram[q * deep:(q + 1) * deep] for q in range(orbs // deep)], 1)
    out_ref[...] = jnp.broadcast_to(packed[None], out_ref.shape)


def rotate_kernel(scale, parts_ref, x_ref, out_ref, gram_ref):
    orbs, rows, lanes = x_ref.shape
    packed = jnp.sum(parts_ref[...], axis=0) * scale
    gram = jnp.concatenate(
        [packed[:, q * orbs:(q + 1) * orbs] for q in range(LANES // orbs)], 0)
    gram_ref[...] = gram
    down = lax.broadcasted_iota(jnp.int32, (orbs, orbs), 0)
    along = lax.broadcasted_iota(jnp.int32, (orbs, orbs), 1)
    eye = jnp.where(down == along, 1.0, 0.0)
    zero = jnp.zeros((orbs, LANES - 2 * orbs), F32)
    work = jnp.concatenate([gram, eye, zero], 1)
    row = lax.broadcasted_iota(jnp.int32, (orbs, LANES), 0)
    pivots = jnp.zeros((orbs, LANES), F32)
    for first in range(0, orbs, PANEL):
        columns = [
            jnp.broadcast_to(work[:, c:c + 1], (orbs, LANES)) for c in range(first, first + PANEL)
        ]
        for k in range(first, first + PANEL):
            column = columns[k - first]
            pivot = column[k:k + 1, :]
            pivots = jnp.where(row == k, pivot, pivots)
            factor = jnp.where(row > k, column * (1.0 / pivot), 0.0)
            work = work - factor * work[k:k + 1, :]
            for c in range(k - first + 1, PANEL):
                columns[c] = columns[c] - factor * columns[c][k:k + 1, :]
    work = work * (1.0 / jnp.sqrt(pivots))
    inverse = work[:, orbs:2 * orbs].astype(BF)
    tall = lax.broadcasted_iota(jnp.int32, (orbs * rows, orbs), 0) // rows
    wide = lax.broadcasted_iota(jnp.int32, (orbs * rows, orbs), 1)
    pick = jnp.where(tall == wide, 1.0, 0.0).astype(BF)
    spread = product(pick, inverse).astype(BF)
    spread = lax.dot_general(spread, pick, (((1,), (1,)), ((), ())), preferred_element_type=F32)
    i = lax.broadcasted_iota(jnp.int32, (orbs * rows, 1), 0) % rows
    j = lax.broadcasted_iota(jnp.int32, (1, orbs * rows), 1) % rows
    spread = jnp.where(i == j, spread, 0.0).astype(BF)
    flat = x_ref[...].reshape(orbs * rows, lanes)
    out_ref[...] = product(spread, flat).astype(BF).reshape(orbs, rows, lanes)


def exchanged(x, axis, by, only=None):
    return lax.ppermute(x, axis, [
        (i, i ^ by) for i in range(lax.axis_size(axis)) if only is None or only(i)])


def body(orbitals):
    orb_count, slab_rows, plane_cells = orbitals.shape
    slabs = lax.axis_size("grid")
    blocks = lax.axis_size("blk")
    assert orb_count == slabs == 4 and slab_rows * slabs == NX and blocks % 2 == 0 and STEPS == 2
    top = slabs // 2
    half = orb_count // 2
    core = lax.axis_index("grid") % 2
    even = lax.axis_index("blk") % 2 == 0
    diagonals, weights = make_tables(slab_rows)

    def shifted(x):
        return lax.ppermute(x, "blk", [(i, (i + 2) % blocks) for i in range(blocks)])

    def relayed(mine, received):
        return exchanged(jnp.where(even, mine, received), "blk", 1)

    def passed_on(x):
        return exchanged(x, "grid", 1, lambda i: i // 2 == i % 2)

    keep = lax.dynamic_slice_in_dim(orbitals, core * half, half, 0)
    give = lax.dynamic_slice_in_dim(orbitals, (1 - core) * half, half, 0)
    keep, give = lax.optimization_barrier((keep, give))
    held = [keep, exchanged(give, "grid", 1)]
    far = [shifted(held[i]) for i in range(2)]
    across = [exchanged(held[i], "grid", top) for i in range(2)]
    near = [relayed(held[i], far[i]) for i in range(2)]
    far_other = [shifted(across[0]), exchanged(far[1], "grid", top)]
    relay, diagonals, weights = lax.optimization_barrier((across[0], diagonals, weights))
    tables = (diagonals, weights)
    near_other = [relayed(relay, far_other[0]), exchanged(near[1], "grid", top)]
    local = held + across
    passed = [give, passed_on(held[0]), passed_on(across[1]), passed_on(across[0])]
    acc = add_block(local, passed, far + far_other, tables, None)
    mine, other = add_block(local, passed, near + near_other, tables, acc)
    other = exchanged(other, "grid", 1)
    chunk = plane_cells // blocks
    if chunk % LANES == 0:
        shape = (blocks, slabs, slab_rows, chunk)
    else:
        shape = (slabs, slab_rows, plane_cells)
    updated = pl.pallas_call(
        functools.partial(combine_kernel, slabs),
        out_shape=jax.ShapeDtypeStruct(shape, BF),
        in_specs=[VMEM, VMEM],
        out_specs=VMEM,
    )(mine, other)
    if chunk % LANES:
        updated = updated.reshape(slabs, slab_rows, blocks, chunk).transpose(2, 0, 1, 3)
    updated = updated.reshape(blocks * slabs, slab_rows, chunk)
    cellwise = lax.all_to_all(updated, ("blk", "grid"), 0, 0, tiled=True)

    devices = blocks * slabs
    cell_count = NX * NY * NZ
    if devices * slab_rows <= 512 and devices % PANEL == 0 and chunk % LANES == 0:
        local = pl.pallas_call(
            gram_kernel,
            out_shape=jax.ShapeDtypeStruct((devices, devices * devices // LANES, LANES), F32),
            in_specs=[VMEM],
            out_specs=VMEM,
        )(cellwise)
        parts = lax.all_to_all(local, ("blk", "grid"), 0, 0, tiled=True)
        return pl.pallas_call(
            functools.partial(rotate_kernel, 1.0 / cell_count),
            out_shape=(
                jax.ShapeDtypeStruct(cellwise.shape, BF),
                jax.ShapeDtypeStruct((devices, devices), F32),
            ),
            in_specs=[VMEM, VMEM],
            out_specs=(VMEM, VMEM),
        )(parts, cellwise)
    flat = cellwise.reshape(devices, slab_rows * chunk)
    local = jnp.dot(flat, flat.T, preferred_element_type=F32)
    intersection = lax.psum(local, ("blk", "grid")) / cell_count
    factor = jnp.linalg.cholesky(intersection)
    identity = jnp.eye(devices, dtype=F32)
    inverse = jax.scipy.linalg.solve_triangular(factor, identity, lower=True).astype(BF)
    rotated = product(inverse, flat).astype(BF)
    return (rotated.reshape(cellwise.shape), intersection)


def solution(mesh):
    in_specs = (P("blk", "grid", None),)
    out_specs = (P(None, "grid", "blk"), P())
    return jax.shard_map(body, mesh=mesh, in_specs=in_specs, out_specs=out_specs, check_vma=False)
```

```python
import functools

import jax
import jax.numpy as jnp
from jax import lax
from jax.experimental import pallas as pl
from jax.experimental.pallas import tpu as pltpu
from jax.sharding import PartitionSpec as P


NX = 64
NY = 64
NZ = 64
STEPS = 2

exchange_fraction = 0.25
screening = 1.0

BF = jnp.bfloat16
F32 = jnp.float32
VMEM = pl.BlockSpec(memory_space=pltpu.VMEM)
SMEM = pl.BlockSpec(memory_space=pltpu.SMEM)
LANES = 128
ROW_PAD = 1
SMALL_VMEM = 10 * 1024 * 1024
QUAD = 4
PANEL = 8


def product(a, b):
    return jnp.dot(a, b, preferred_element_type=F32)


def sines(rows, columns, length):
    angle = jnp.pi * (rows + 1.0) * (columns + 1.0) / (length + 1)
    return jnp.sqrt(2.0 / (length + 1)) * jnp.sin(angle)


def eigen_values(index, length):
    return 2.0 - 2.0 * jnp.cos(jnp.pi * (index + 1.0) / (length + 1))


def table_kernel(slab_rows, diag_ref, weight_ref):
    size = diag_ref.shape[1]
    copies = size // NX
    grid_index = lax.axis_index("grid")

    def cells_of(position):
        slab = position // slab_rows
        start = jnp.zeros_like(position)
        for r in range(NX // slab_rows):
            start = jnp.where(slab == r, (grid_index ^ r) * slab_rows, start)
        return start + position % slab_rows

    shape = (NX, LANES)
    down = lax.broadcasted_iota(jnp.int32, shape, 0)
    along = lax.broadcasted_iota(jnp.int32, shape, 1) % NX
    pairs = (
        (down, along),
        (down, cells_of(along)),
        (cells_of(down), along),
    )
    same = (
        lax.broadcasted_iota(jnp.int32, (NX, size), 1) // NX
    )
    for i, (row, column) in enumerate(pairs):
        table = sines(row.astype(F32), column.astype(F32), NX)
        table = jnp.concatenate([table] * (size // LANES), 1)
        for c in range(copies):
            diag_ref[i, c * NX:(c + 1) * NX, :] = jnp.where(same == c, table, 0.0).astype(BF)
    lam = eigen_values(down.astype(F32), NX)
    plane = screening + lam + eigen_values(along.astype(F32), NZ)
    for k in range(NX):
        weight_ref[k * NY:(k + 1) * NY, :] = 1.0 / (lam[k:k + 1, :] + plane)


def make_tables(slab_rows):
    size = QUAD * NX
    return pl.pallas_call(
        functools.partial(table_kernel, slab_rows),
        out_shape=(
            jax.ShapeDtypeStruct((3, size, size), BF),
            jax.ShapeDtypeStruct((NX * NY, LANES), F32),
        ),
        out_specs=(VMEM, VMEM),
        compiler_params=pltpu.CompilerParams(vmem_limit_bytes=SMALL_VMEM),
        cost_estimate=pl.CostEstimate(flops=1 << 28, bytes_accessed=3 << 20, transcendentals=0),
    )()


def block_kernel(slabs, final, rest):
    grid_index = lax.axis_index("grid")
    core, chip = grid_index % 2, grid_index // 2
    local = rest[:slabs]
    passed = rest[slabs:2 * slabs]
    src = rest[2 * slabs:3 * slabs]
    tab_ref, w_ref = rest[3 * slabs:3 * slabs + 2]
    rest = rest[3 * slabs + 2:]
    if final:
        acc_ref, keep_ref, send_ref, grouped_ref, work_ref = rest
    else:
        out_ref, grouped_ref, work_ref = rest
    owns = local[0].shape[0]
    count = src[0].shape[0]
    halves = owns * count * NZ // LANES
    width = QUAD * NZ
    pitch = work_ref.shape[1] // NY

    def tile(refs, j, off, size):
        return jnp.concatenate([r[j, :, pl.ds(off, size)] for r in refs], 0)

    def own_tile(o, off, size):
        return jnp.where(core == chip, tile(local, o, off, size), tile(passed, o, off, size))

    def forward(t):
        off = t * width
        at = t * QUAD * NX
        mine = [own_tile(o, off, width) for o in range(owns)]
        others = [tile(src, j, off, width) for j in range(count)]
        pairs = [m * other for m in mine for other in others]
        cut = [slice(q * NZ, (q + 1) * NZ) for q in range(QUAD)]
        density = jnp.concatenate(
            [jnp.concatenate([p[:, c] for p in pairs], 1) for c in cut], 0)
        grouped_ref[pl.ds(at, QUAD * NX), :] = jnp.concatenate(
            [jnp.concatenate([o[:, c] for o in others], 1) for c in cut], 0)
        first = product(density, tab_ref[0]).astype(BF)
        modes = product(tab_ref[1], first)
        for q in range(QUAD):
            to = (t * QUAD + q) * pitch
            for h in range(halves):
                work_ref[h, pl.ds(to, NX), :] = modes[q * NX:(q + 1) * NX, h * LANES:(h + 1) * LANES]

    def solve(t):
        at = t * QUAD * NY
        modes = jnp.concatenate([
            jnp.concatenate(
                [work_ref[h, pl.ds(t * QUAD + q, NY, stride=pitch), :] for h in range(halves)], 1)
            for q in range(QUAD)], 0).astype(BF)
        weights = jnp.concatenate([w_ref[pl.ds(at, QUAD * NY), :]] * halves, 1)
        scaled = (product(tab_ref[0], modes) * weights).astype(BF)
        back = product(tab_ref[0], scaled)
        for q in range(QUAD):
            for h in range(halves):
                work_ref[h, pl.ds(t * QUAD + q, NY, stride=pitch), :] = (
                    back[q * NY:(q + 1) * NY, h * LANES:(h + 1) * LANES])

    lane = lax.broadcasted_iota(jnp.int32, (NX, LANES), 1)

    def backward(t):
        at = t * QUAD * NX
        modes = jnp.concatenate([
            jnp.concatenate(
                [work_ref[h, pl.ds((t * QUAD + q) * pitch, NX), :] for h in range(halves)], 1)
            for q in range(QUAD)], 0).astype(BF)
        third = product(tab_ref[2], modes).astype(BF)
        potential = product(third, tab_ref[0])
        factor = grouped_ref[pl.ds(at, QUAD * NX), :].astype(F32)
        totals = []
        for o in range(owns):
            terms = potential[:, o * LANES:(o + 1) * LANES] * factor
            totals.append(terms + pltpu.roll(terms, NZ, 1))
        for q in range(0, QUAD, LANES // NZ):
            off = (t * QUAD + q) * NZ
            exchange = [
                jnp.where(lane < NZ, x[q * NX:(q + 1) * NX], x[(q + 1) * NX:(q + 2) * NX])
                for x in totals
            ]
            if not final:
                for o in range(owns):
                    out_ref[o, :, pl.ds(off, LANES)] = exchange[o]
                continue
            exchange = [
                exchange_fraction * (x + acc_ref[o, :, pl.ds(off, LANES)])
                for o, x in enumerate(exchange)
            ]
            own = [own_tile(o, off, LANES) for o in range(owns)]
            first = core == 0
            own = jnp.where(first, own[0], own[1]).astype(F32)
            keep_ref[:, pl.ds(off, LANES)] = own - jnp.where(first, exchange[0], exchange[1])
            send_ref[:, pl.ds(off, LANES)] = (
                jnp.where(first, exchange[1], exchange[0]).astype(send_ref.dtype))

    for step, trips in ((forward, NY // QUAD), (solve, NX // QUAD), (backward, NY // QUAD)):
        for t in range(trips):
            step(t)


def add_block(local, passed, src, tables, acc):
    slabs = len(local)
    owns, _, cells = local[0].shape
    count = src[0].shape[0]
    assert count * NZ == LANES and owns == 2
    final = acc is not None
    lead = () if acc is None else (acc,)
    flops = 12 * owns * count * NX * NY * NZ * NZ * 4
    if final:
        out_shape = (
            jax.ShapeDtypeStruct((NX, cells), F32), jax.ShapeDtypeStruct((NX, cells), BF))
    else:
        out_shape = jax.ShapeDtypeStruct((owns, NX, cells), F32)
    return pl.pallas_call(
        lambda *refs: block_kernel(slabs, final, refs),
        out_shape=out_shape,
        in_specs=[VMEM] * (3 * slabs + 2 + len(lead)),
        out_specs=(VMEM, VMEM) if final else VMEM,
        scratch_shapes=[
            pltpu.VMEM((NY * NX, count * NZ), BF),
            pltpu.VMEM((owns * count * NZ // LANES, NY * (NX + ROW_PAD), LANES), F32),
        ],
        compiler_params=pltpu.CompilerParams(vmem_limit_bytes=24 * 1024 * 1024),
        cost_estimate=pl.CostEstimate(flops=flops, bytes_accessed=8 << 20, transcendentals=0),
    )(*local, *passed, *src, *tables, *lead)


def combine_kernel(slabs, keep_ref, part_ref, out_ref):
    grid_index = lax.axis_index("grid")
    rows = keep_ref.shape[0] // slabs
    for r in range(slabs):
        other = (r ^ 1) * rows
        updated = keep_ref[r * rows:(r + 1) * rows] - part_ref[other:other + rows].astype(F32)
        updated = updated.astype(BF)
        if len(out_ref.shape) == 3:
            out_ref[grid_index ^ r] = updated
            continue
        share = out_ref.shape[3]
        for b in range(out_ref.shape[0]):
            out_ref[b, grid_index ^ r] = updated[:, b * share:(b + 1) * share]


def gram_kernel(x_ref, out_ref):
    orbs, rows, lanes = x_ref.shape
    flat = x_ref[...].reshape(orbs * rows, lanes)
    full = lax.dot_general(flat, flat, (((1,), (1,)), ((), ())), preferred_element_type=F32)
    down = lax.broadcasted_iota(jnp.int32, (rows, orbs * rows), 0)
    along = lax.broadcasted_iota(jnp.int32, (rows, orbs * rows), 1)
    same = down == along % rows
    half = [
        jnp.sum(jnp.where(same, full[o * rows:(o + 1) * rows], 0.0), axis=0, keepdims=True)
        for o in range(orbs)
    ]
    half = jnp.concatenate(half, 0)
    gram = jnp.sum(half.T.reshape(orbs, rows, orbs), axis=1)
    deep = orbs * orbs // LANES
    packed = jnp.concatenate([gram[q * deep:(q + 1) * deep] for q in range(orbs // deep)], 1)
    out_ref[...] = jnp.broadcast_to(packed[None], out_ref.shape)


def rotate_kernel(scale, parts_ref, x_ref, out_ref, gram_ref):
    orbs, rows, lanes = x_ref.shape
    packed = jnp.sum(parts_ref[...], axis=0) * scale
    gram = jnp.concatenate(
        [packed[:, q * orbs:(q + 1) * orbs] for q in range(LANES // orbs)], 0)
    gram_ref[...] = gram
    down = lax.broadcasted_iota(jnp.int32, (orbs, orbs), 0)
    along = lax.broadcasted_iota(jnp.int32, (orbs, orbs), 1)
    eye = jnp.where(down == along, 1.0, 0.0)
    zero = jnp.zeros((orbs, LANES - 2 * orbs), F32)
    work = jnp.concatenate([gram, eye, zero], 1)
    row = lax.broadcasted_iota(jnp.int32, (orbs, LANES), 0)
    pivots = jnp.zeros((orbs, LANES), F32)
    for first in range(0, orbs, PANEL):
        columns = [
            jnp.broadcast_to(work[:, c:c + 1], (orbs, LANES)) for c in range(first, first + PANEL)
        ]
        for k in range(first, first + PANEL):
            column = columns[k - first]
            pivot = column[k:k + 1, :]
            pivots = jnp.where(row == k, pivot, pivots)
            factor = jnp.where(row > k, column * (1.0 / pivot), 0.0)
            work = work - factor * work[k:k + 1, :]
            for c in range(k - first + 1, PANEL):
                columns[c] = columns[c] - factor * columns[c][k:k + 1, :]
    work = work * (1.0 / jnp.sqrt(pivots))
    inverse = work[:, orbs:2 * orbs].astype(BF)
    tall = lax.broadcasted_iota(jnp.int32, (orbs * rows, orbs), 0) // rows
    wide = lax.broadcasted_iota(jnp.int32, (orbs * rows, orbs), 1)
    pick = jnp.where(tall == wide, 1.0, 0.0).astype(BF)
    spread = product(pick, inverse).astype(BF)
    spread = lax.dot_general(spread, pick, (((1,), (1,)), ((), ())), preferred_element_type=F32)
    i = lax.broadcasted_iota(jnp.int32, (orbs * rows, 1), 0) % rows
    j = lax.broadcasted_iota(jnp.int32, (1, orbs * rows), 1) % rows
    spread = jnp.where(i == j, spread, 0.0).astype(BF)
    flat = x_ref[...].reshape(orbs * rows, lanes)
    out_ref[...] = product(spread, flat).astype(BF).reshape(orbs, rows, lanes)


def exchanged(x, axis, by, only=None):
    return lax.ppermute(x, axis, [
        (i, i ^ by) for i in range(lax.axis_size(axis)) if only is None or only(i)])


def body(orbitals):
    orb_count, slab_rows, plane_cells = orbitals.shape
    slabs = lax.axis_size("grid")
    blocks = lax.axis_size("blk")
    assert orb_count == slabs == 4 and slab_rows * slabs == NX and blocks % 2 == 0 and STEPS == 2
    top = slabs // 2
    half = orb_count // 2
    core = lax.axis_index("grid") % 2
    even = lax.axis_index("blk") % 2 == 0
    diagonals, weights = make_tables(slab_rows)

    def shifted(x):
        return lax.ppermute(x, "blk", [(i, (i + 2) % blocks) for i in range(blocks)])

    def relayed(mine, received):
        return exchanged(jnp.where(even, mine, received), "blk", 1)

    def passed_on(x):
        return exchanged(x, "grid", 1, lambda i: i // 2 == i % 2)

    keep = lax.dynamic_slice_in_dim(orbitals, core * half, half, 0)
    give = lax.dynamic_slice_in_dim(orbitals, (1 - core) * half, half, 0)
    keep, give = lax.optimization_barrier((keep, give))
    held = [keep, exchanged(give, "grid", 1)]
    far = [shifted(held[i]) for i in range(2)]
    across = [exchanged(held[i], "grid", top) for i in range(2)]
    near = [relayed(held[i], far[i]) for i in range(2)]
    far_other = [shifted(across[0]), exchanged(far[1], "grid", top)]
    relay, diagonals, weights = lax.optimization_barrier((across[0], diagonals, weights))
    tables = (diagonals, weights)
    near_other = [relayed(relay, far_other[0]), exchanged(near[1], "grid", top)]
    local = held + across
    passed = [give, passed_on(held[0]), passed_on(across[1]), passed_on(across[0])]
    acc = add_block(local, passed, far + far_other, tables, None)
    mine, other = add_block(local, passed, near + near_other, tables, acc)
    other = exchanged(other, "grid", 1)
    chunk = plane_cells // blocks
    if chunk % LANES == 0:
        shape = (blocks, slabs, slab_rows, chunk)
    else:
        shape = (slabs, slab_rows, plane_cells)
    updated = pl.pallas_call(
        functools.partial(combine_kernel, slabs),
        out_shape=jax.ShapeDtypeStruct(shape, BF),
        in_specs=[VMEM, VMEM],
        out_specs=VMEM,
        compiler_params=pltpu.CompilerParams(vmem_limit_bytes=SMALL_VMEM),
    )(mine, other)
    if chunk % LANES:
        updated = updated.reshape(slabs, slab_rows, blocks, chunk).transpose(2, 0, 1, 3)
    updated = updated.reshape(blocks * slabs, slab_rows, chunk)
    cellwise = lax.all_to_all(updated, ("blk", "grid"), 0, 0, tiled=True)

    devices = blocks * slabs
    cell_count = NX * NY * NZ
    if devices * slab_rows <= 512 and devices % PANEL == 0 and chunk % LANES == 0:
        local = pl.pallas_call(
            gram_kernel,
            out_shape=jax.ShapeDtypeStruct((devices, devices * devices // LANES, LANES), F32),
            in_specs=[VMEM],
            out_specs=VMEM,
            compiler_params=pltpu.CompilerParams(vmem_limit_bytes=SMALL_VMEM),
        )(cellwise)
        parts = lax.all_to_all(local, ("blk", "grid"), 0, 0, tiled=True)
        return pl.pallas_call(
            functools.partial(rotate_kernel, 1.0 / cell_count),
            out_shape=(
                jax.ShapeDtypeStruct(cellwise.shape, BF),
                jax.ShapeDtypeStruct((devices, devices), F32),
            ),
            in_specs=[VMEM, VMEM],
            out_specs=(VMEM, VMEM),
            compiler_params=pltpu.CompilerParams(vmem_limit_bytes=SMALL_VMEM),
        )(parts, cellwise)
    flat = cellwise.reshape(devices, slab_rows * chunk)
    local = jnp.dot(flat, flat.T, preferred_element_type=F32)
    intersection = lax.psum(local, ("blk", "grid")) / cell_count
    factor = jnp.linalg.cholesky(intersection)
    identity = jnp.eye(devices, dtype=F32)
    inverse = jax.scipy.linalg.solve_triangular(factor, identity, lower=True).astype(BF)
    rotated = product(inverse, flat).astype(BF)
    return (rotated.reshape(cellwise.shape), intersection)


def solution(mesh):
    in_specs = (P("blk", "grid", None),)
    out_specs = (P(None, "grid", "blk"), P())
    return jax.shard_map(body, mesh=mesh, in_specs=in_specs, out_specs=out_specs, check_vma=False)
```

```python
import functools

import jax
import jax.numpy as jnp
from jax import lax
from jax.experimental import pallas as pl
from jax.experimental.pallas import tpu as pltpu
from jax.sharding import PartitionSpec as P


NX = 64
NY = 64
NZ = 64
STEPS = 2

exchange_fraction = 0.25
screening = 1.0

BF = jnp.bfloat16
F32 = jnp.float32
VMEM = pl.BlockSpec(memory_space=pltpu.VMEM)
SMEM = pl.BlockSpec(memory_space=pltpu.SMEM)
LANES = 128
ROW_PAD = 1
SMALL_VMEM = 10 * 1024 * 1024
QUAD = 4
PANEL = 8


def product(a, b):
    return jnp.dot(a, b, preferred_element_type=F32)


def sines(rows, columns, length):
    angle = jnp.pi * (rows + 1.0) * (columns + 1.0) / (length + 1)
    return jnp.sqrt(2.0 / (length + 1)) * jnp.sin(angle)


def eigen_values(index, length):
    return 2.0 - 2.0 * jnp.cos(jnp.pi * (index + 1.0) / (length + 1))


def table_kernel(slab_rows, diag_ref, weight_ref):
    size = diag_ref.shape[1]
    copies = size // NX
    grid_index = lax.axis_index("grid")

    def cells_of(position):
        slab = position // slab_rows
        start = jnp.zeros_like(position)
        for r in range(NX // slab_rows):
            start = jnp.where(slab == r, (grid_index ^ r) * slab_rows, start)
        return start + position % slab_rows

    shape = (NX, LANES)
    down = lax.broadcasted_iota(jnp.int32, shape, 0)
    along = lax.broadcasted_iota(jnp.int32, shape, 1) % NX
    pairs = (
        (down, along),
        (down, cells_of(along)),
        (cells_of(down), along),
    )
    same = (
        lax.broadcasted_iota(jnp.int32, (NX, size), 1) // NX
    )
    for i, (row, column) in enumerate(pairs):
        table = sines(row.astype(F32), column.astype(F32), NX)
        table = jnp.concatenate([table] * (size // LANES), 1)
        for c in range(copies):
            block = jnp.where(same == c, table, 0.0).astype(BF)
            diag_ref[i, c * NX:(c + 1) * NX, :] = block
            if i == 0:
                block = (block.astype(F32) * exchange_fraction).astype(BF)
                diag_ref[len(pairs), c * NX:(c + 1) * NX, :] = block
    lam = eigen_values(down.astype(F32), NX)
    plane = screening + lam + eigen_values(along.astype(F32), NZ)
    for k in range(NX):
        weight_ref[k * NY:(k + 1) * NY, :] = 1.0 / (lam[k:k + 1, :] + plane)


def make_tables(slab_rows):
    size = QUAD * NX
    return pl.pallas_call(
        functools.partial(table_kernel, slab_rows),
        out_shape=(
            jax.ShapeDtypeStruct((4, size, size), BF),
            jax.ShapeDtypeStruct((NX * NY, LANES), F32),
        ),
        out_specs=(VMEM, VMEM),
        compiler_params=pltpu.CompilerParams(vmem_limit_bytes=SMALL_VMEM),
        cost_estimate=pl.CostEstimate(flops=1 << 28, bytes_accessed=3 << 20, transcendentals=0),
    )()


def block_kernel(slabs, final, rest):
    grid_index = lax.axis_index("grid")
    core, chip = grid_index % 2, grid_index // 2
    local = rest[:slabs]
    passed = rest[slabs:2 * slabs]
    src = rest[2 * slabs:3 * slabs]
    tab_ref, w_ref = rest[3 * slabs:3 * slabs + 2]
    rest = rest[3 * slabs + 2:]
    if final:
        acc_ref, keep_ref, send_ref, grouped_ref, work_ref = rest
    else:
        out_ref, grouped_ref, work_ref = rest
    owns = local[0].shape[0]
    count = src[0].shape[0]
    halves = owns * count * NZ // LANES
    pitch = work_ref.shape[1] // NY

    low = lax.broadcasted_iota(jnp.int32, (NX, LANES), 1) < NZ
    low16 = lax.broadcasted_iota(jnp.int16, (NX, LANES), 1) < NZ

    def swapped(x):
        return jnp.concatenate([x[:, NZ:], x[:, :NZ]], 1)

    def tile(refs, j, off):
        return jnp.concatenate([r[j, :, pl.ds(off, LANES)] for r in refs], 0)

    def own_tile(o, off):
        j = (core + o) % owns
        return jnp.where(core == chip, tile(local, j, off), tile(passed, j, off))

    def forward(t):
        at = t * QUAD * NX
        rows_d, rows_s = [], []
        for q in range(0, QUAD, LANES // NZ):
            off = (t * QUAD + q) * NZ
            a, b = tile(src, 0, off), tile(src, 1, off)
            mixed = swapped(jnp.where(low16, b, a))
            pair = [jnp.where(low16, a, mixed), jnp.where(low16, mixed, b)]
            rows_s += pair
            wide = []
            for o in range(owns):
                mine = own_tile(o, off)
                turned = swapped(mine)
                wide.append([jnp.where(low16, mine, turned), jnp.where(low16, turned, mine)])
            for y in range(2):
                rows_d.append(jnp.concatenate([w[y] * pair[y] for w in wide], 1))
        grouped_ref[pl.ds(at, QUAD * NX), :] = jnp.concatenate(rows_s, 0)
        first = product(jnp.concatenate(rows_d, 0), tab_ref[0]).astype(BF)
        modes = product(tab_ref[1], first)
        for q in range(QUAD):
            to = (t * QUAD + q) * pitch
            for h in range(halves):
                work_ref[h, pl.ds(to, NX), :] = modes[q * NX:(q + 1) * NX, h * LANES:(h + 1) * LANES]

    def solve(t):
        at = t * QUAD * NY
        modes = jnp.concatenate([
            jnp.concatenate(
                [work_ref[h, pl.ds(t * QUAD + q, NY, stride=pitch), :] for h in range(halves)], 1)
            for q in range(QUAD)], 0).astype(BF)
        weights = jnp.concatenate([w_ref[pl.ds(at, QUAD * NY), :]] * halves, 1)
        scaled = (product(tab_ref[0], modes) * weights).astype(BF)
        back = product(tab_ref[0], scaled)
        for q in range(QUAD):
            for h in range(halves):
                work_ref[h, pl.ds(t * QUAD + q, NY, stride=pitch), :] = (
                    back[q * NY:(q + 1) * NY, h * LANES:(h + 1) * LANES])

    def backward(t):
        at = t * QUAD * NX
        modes = jnp.concatenate([
            jnp.concatenate(
                [work_ref[h, pl.ds((t * QUAD + q) * pitch, NX), :] for h in range(halves)], 1)
            for q in range(QUAD)], 0).astype(BF)
        third = product(tab_ref[2], modes).astype(BF)
        potential = product(third, tab_ref[3])
        for q in range(0, QUAD, LANES // NZ):
            off = (t * QUAD + q) * NZ
            factor = [
                grouped_ref[pl.ds(at + (q + y) * NX, NX), :].astype(F32) for y in range(2)
            ]
            for o in range(owns):
                a, b = [
                    potential[(q + y) * NX:(q + y + 1) * NX, o * LANES:(o + 1) * LANES] * factor[y]
                    for y in range(2)
                ]
                exchange = jnp.where(low, a, b) + pltpu.roll(jnp.where(low, b, a), NZ, 1)
                if not final:
                    out_ref[o, :, pl.ds(off, LANES)] = exchange
                    continue
                exchange = exchange + acc_ref[o, :, pl.ds(off, LANES)]
                if o == 0:
                    keep_ref[:, pl.ds(off, LANES)] = own_tile(0, off).astype(F32) - exchange
                else:
                    send_ref[:, pl.ds(off, LANES)] = exchange.astype(send_ref.dtype)

    for step, trips in ((forward, NY // QUAD), (solve, NX // QUAD), (backward, NY // QUAD)):
        for t in range(trips):
            step(t)


def add_block(local, passed, src, tables, acc):
    slabs = len(local)
    owns, _, cells = local[0].shape
    count = src[0].shape[0]
    assert count * NZ == LANES and owns == 2
    final = acc is not None
    lead = () if acc is None else (acc,)
    flops = 12 * owns * count * NX * NY * NZ * NZ * 4
    if final:
        out_shape = (
            jax.ShapeDtypeStruct((NX, cells), F32), jax.ShapeDtypeStruct((NX, cells), BF))
    else:
        out_shape = jax.ShapeDtypeStruct((owns, NX, cells), F32)
    return pl.pallas_call(
        lambda *refs: block_kernel(slabs, final, refs),
        out_shape=out_shape,
        in_specs=[VMEM] * (3 * slabs + 2 + len(lead)),
        out_specs=(VMEM, VMEM) if final else VMEM,
        scratch_shapes=[
            pltpu.VMEM((NY * NX, count * NZ), BF),
            pltpu.VMEM((owns * count * NZ // LANES, NY * (NX + ROW_PAD), LANES), F32),
        ],
        compiler_params=pltpu.CompilerParams(vmem_limit_bytes=24 * 1024 * 1024),
        cost_estimate=pl.CostEstimate(flops=flops, bytes_accessed=8 << 20, transcendentals=0),
    )(*local, *passed, *src, *tables, *lead)


def combine_kernel(slabs, keep_ref, part_ref, out_ref):
    grid_index = lax.axis_index("grid")
    rows = keep_ref.shape[0] // slabs
    for r in range(slabs):
        other = (r ^ 1) * rows
        updated = keep_ref[r * rows:(r + 1) * rows] - part_ref[other:other + rows].astype(F32)
        updated = updated.astype(BF)
        if len(out_ref.shape) == 3:
            out_ref[grid_index ^ r] = updated
            continue
        share = out_ref.shape[3]
        for b in range(out_ref.shape[0]):
            out_ref[b, grid_index ^ r] = updated[:, b * share:(b + 1) * share]


def gram_kernel(x_ref, out_ref):
    orbs, rows, lanes = x_ref.shape
    flat = x_ref[...].reshape(orbs * rows, lanes)
    full = lax.dot_general(flat, flat, (((1,), (1,)), ((), ())), preferred_element_type=F32)
    down = lax.broadcasted_iota(jnp.int32, (rows, orbs * rows), 0)
    along = lax.broadcasted_iota(jnp.int32, (rows, orbs * rows), 1)
    same = down == along % rows
    half = [
        jnp.sum(jnp.where(same, full[o * rows:(o + 1) * rows], 0.0), axis=0, keepdims=True)
        for o in range(orbs)
    ]
    half = jnp.concatenate(half, 0)
    gram = jnp.sum(half.T.reshape(orbs, rows, orbs), axis=1)
    deep = orbs * orbs // LANES
    packed = jnp.concatenate([gram[q * deep:(q + 1) * deep] for q in range(orbs // deep)], 1)
    out_ref[...] = jnp.broadcast_to(packed[None], out_ref.shape)


def rotate_kernel(scale, parts_ref, x_ref, out_ref, gram_ref):
    orbs, rows, lanes = x_ref.shape
    packed = jnp.sum(parts_ref[...], axis=0) * scale
    gram = jnp.concatenate(
        [packed[:, q * orbs:(q + 1) * orbs] for q in range(LANES // orbs)], 0)
    gram_ref[...] = gram
    down = lax.broadcasted_iota(jnp.int32, (orbs, orbs), 0)
    along = lax.broadcasted_iota(jnp.int32, (orbs, orbs), 1)
    eye = jnp.where(down == along, 1.0, 0.0)
    zero = jnp.zeros((orbs, LANES - 2 * orbs), F32)
    work = jnp.concatenate([gram, eye, zero], 1)
    row = lax.broadcasted_iota(jnp.int32, (orbs, LANES), 0)
    pivots = jnp.zeros((orbs, LANES), F32)
    for first in range(0, orbs, PANEL):
        columns = [
            jnp.broadcast_to(work[:, c:c + 1], (orbs, LANES)) for c in range(first, first + PANEL)
        ]
        for k in range(first, first + PANEL):
            column = columns[k - first]
            pivot = column[k:k + 1, :]
            pivots = jnp.where(row == k, pivot, pivots)
            factor = jnp.where(row > k, column * (1.0 / pivot), 0.0)
            work = work - factor * work[k:k + 1, :]
            for c in range(k - first + 1, PANEL):
                columns[c] = columns[c] - factor * columns[c][k:k + 1, :]
    work = work * (1.0 / jnp.sqrt(pivots))
    inverse = work[:, orbs:2 * orbs].astype(BF)
    tall = lax.broadcasted_iota(jnp.int32, (orbs * rows, orbs), 0) // rows
    wide = lax.broadcasted_iota(jnp.int32, (orbs * rows, orbs), 1)
    pick = jnp.where(tall == wide, 1.0, 0.0).astype(BF)
    spread = product(pick, inverse).astype(BF)
    spread = lax.dot_general(spread, pick, (((1,), (1,)), ((), ())), preferred_element_type=F32)
    i = lax.broadcasted_iota(jnp.int32, (orbs * rows, 1), 0) % rows
    j = lax.broadcasted_iota(jnp.int32, (1, orbs * rows), 1) % rows
    spread = jnp.where(i == j, spread, 0.0).astype(BF)
    flat = x_ref[...].reshape(orbs * rows, lanes)
    out_ref[...] = product(spread, flat).astype(BF).reshape(orbs, rows, lanes)


def exchanged(x, axis, by, only=None):
    return lax.ppermute(x, axis, [
        (i, i ^ by) for i in range(lax.axis_size(axis)) if only is None or only(i)])


def body(orbitals):
    orb_count, slab_rows, plane_cells = orbitals.shape
    slabs = lax.axis_size("grid")
    blocks = lax.axis_size("blk")
    assert orb_count == slabs == 4 and slab_rows * slabs == NX and blocks % 2 == 0 and STEPS == 2
    top = slabs // 2
    half = orb_count // 2
    core = lax.axis_index("grid") % 2
    even = lax.axis_index("blk") % 2 == 0
    diagonals, weights = make_tables(slab_rows)

    def shifted(x):
        return lax.ppermute(x, "blk", [(i, (i + 2) % blocks) for i in range(blocks)])

    def relayed(mine, received):
        return exchanged(jnp.where(even, mine, received), "blk", 1)

    def passed_on(x):
        return exchanged(x, "grid", 1, lambda i: i // 2 == i % 2)

    keep = lax.dynamic_slice_in_dim(orbitals, core * half, half, 0)
    give = lax.dynamic_slice_in_dim(orbitals, (1 - core) * half, half, 0)
    keep, give = lax.optimization_barrier((keep, give))
    held = [keep, exchanged(give, "grid", 1)]
    far = [shifted(held[i]) for i in range(2)]
    across = [exchanged(held[i], "grid", top) for i in range(2)]
    near = [relayed(held[i], far[i]) for i in range(2)]
    far_other = [shifted(across[0]), exchanged(far[1], "grid", top)]
    relay, diagonals, weights = lax.optimization_barrier((across[0], diagonals, weights))
    tables = (diagonals, weights)
    near_other = [relayed(relay, far_other[0]), exchanged(near[1], "grid", top)]
    local = held + across
    passed = [give, passed_on(held[0]), passed_on(across[1]), passed_on(across[0])]
    acc = add_block(local, passed, far + far_other, tables, None)
    mine, other = add_block(local, passed, near + near_other, tables, acc)
    other = exchanged(other, "grid", 1)
    chunk = plane_cells // blocks
    if chunk % LANES == 0:
        shape = (blocks, slabs, slab_rows, chunk)
    else:
        shape = (slabs, slab_rows, plane_cells)
    updated = pl.pallas_call(
        functools.partial(combine_kernel, slabs),
        out_shape=jax.ShapeDtypeStruct(shape, BF),
        in_specs=[VMEM, VMEM],
        out_specs=VMEM,
        compiler_params=pltpu.CompilerParams(vmem_limit_bytes=SMALL_VMEM),
    )(mine, other)
    if chunk % LANES:
        updated = updated.reshape(slabs, slab_rows, blocks, chunk).transpose(2, 0, 1, 3)
    updated = updated.reshape(blocks * slabs, slab_rows, chunk)
    cellwise = lax.all_to_all(updated, ("blk", "grid"), 0, 0, tiled=True)

    devices = blocks * slabs
    cell_count = NX * NY * NZ
    if devices * slab_rows <= 512 and devices % PANEL == 0 and chunk % LANES == 0:
        local = pl.pallas_call(
            gram_kernel,
            out_shape=jax.ShapeDtypeStruct((devices, devices * devices // LANES, LANES), F32),
            in_specs=[VMEM],
            out_specs=VMEM,
            compiler_params=pltpu.CompilerParams(vmem_limit_bytes=SMALL_VMEM),
        )(cellwise)
        parts = lax.all_to_all(local, ("blk", "grid"), 0, 0, tiled=True)
        return pl.pallas_call(
            functools.partial(rotate_kernel, 1.0 / cell_count),
            out_shape=(
                jax.ShapeDtypeStruct(cellwise.shape, BF),
                jax.ShapeDtypeStruct((devices, devices), F32),
            ),
            in_specs=[VMEM, VMEM],
            out_specs=(VMEM, VMEM),
            compiler_params=pltpu.CompilerParams(vmem_limit_bytes=SMALL_VMEM),
        )(parts, cellwise)
    flat = cellwise.reshape(devices, slab_rows * chunk)
    local = jnp.dot(flat, flat.T, preferred_element_type=F32)
    intersection = lax.psum(local, ("blk", "grid")) / cell_count
    factor = jnp.linalg.cholesky(intersection)
    identity = jnp.eye(devices, dtype=F32)
    inverse = jax.scipy.linalg.solve_triangular(factor, identity, lower=True).astype(BF)
    rotated = product(inverse, flat).astype(BF)
    return (rotated.reshape(cellwise.shape), intersection)


def solution(mesh):
    in_specs = (P("blk", "grid", None),)
    out_specs = (P(None, "grid", "blk"), P())
    return jax.shard_map(body, mesh=mesh, in_specs=in_specs, out_specs=out_specs, check_vma=False)
```

```python
import functools

import jax
import jax.numpy as jnp
from jax import lax
from jax.experimental import pallas as pl
from jax.experimental.pallas import tpu as pltpu
from jax.sharding import PartitionSpec as P


NX = 64
NY = 64
NZ = 64
STEPS = 2

exchange_fraction = 0.25
screening = 1.0

BF = jnp.bfloat16
F32 = jnp.float32
VMEM = pl.BlockSpec(memory_space=pltpu.VMEM)
SMEM = pl.BlockSpec(memory_space=pltpu.SMEM)
LANES = 128
ROW_PAD = 1
SMALL_VMEM = 10 * 1024 * 1024
QUAD = 4
PANEL = 8


def product(a, b):
    return jnp.dot(a, b, preferred_element_type=F32)


def sines(rows, columns, length):
    angle = jnp.pi * (rows + 1.0) * (columns + 1.0) / (length + 1)
    return jnp.sqrt(2.0 / (length + 1)) * jnp.sin(angle)


def eigen_values(index, length):
    return 2.0 - 2.0 * jnp.cos(jnp.pi * (index + 1.0) / (length + 1))


def table_kernel(slab_rows, diag_ref, weight_ref):
    size = diag_ref.shape[1]
    copies = size // NX
    grid_index = lax.axis_index("grid")

    def cells_of(position):
        slab = position // slab_rows
        start = jnp.zeros_like(position)
        for r in range(NX // slab_rows):
            start = jnp.where(slab == r, (grid_index ^ r) * slab_rows, start)
        return start + position % slab_rows

    shape = (NX, LANES)
    down = lax.broadcasted_iota(jnp.int32, shape, 0)
    along = lax.broadcasted_iota(jnp.int32, shape, 1) % NX
    pairs = (
        (down, along),
        (down, cells_of(along)),
        (cells_of(down), along),
    )
    same = (
        lax.broadcasted_iota(jnp.int32, (NX, size), 1) // NX
    )
    for i, (row, column) in enumerate(pairs):
        table = sines(row.astype(F32), column.astype(F32), NX)
        table = jnp.concatenate([table] * (size // LANES), 1)
        for c in range(copies):
            block = jnp.where(same == c, table, 0.0).astype(BF)
            diag_ref[i, c * NX:(c + 1) * NX, :] = block
            if i == 0:
                block = (block.astype(F32) * exchange_fraction).astype(BF)
                diag_ref[len(pairs), c * NX:(c + 1) * NX, :] = block
    lam = eigen_values(down.astype(F32), NX)
    plane = screening + lam + eigen_values(along.astype(F32), NZ)
    for k in range(NX):
        weight_ref[k * NY:(k + 1) * NY, :] = 1.0 / (lam[k:k + 1, :] + plane)


def make_tables(slab_rows):
    size = QUAD * NX
    return pl.pallas_call(
        functools.partial(table_kernel, slab_rows),
        out_shape=(
            jax.ShapeDtypeStruct((4, size, size), BF),
            jax.ShapeDtypeStruct((NX * NY, LANES), F32),
        ),
        out_specs=(VMEM, VMEM),
        compiler_params=pltpu.CompilerParams(vmem_limit_bytes=SMALL_VMEM),
        cost_estimate=pl.CostEstimate(flops=1 << 28, bytes_accessed=3 << 20, transcendentals=0),
    )()


def rows_of(refs):
    return [(ref, j) for ref in refs for j in range(ref.shape[0])]


def block_kernel(counts, final, rest):
    grid_index = lax.axis_index("grid")
    core, chip = grid_index % 2, grid_index // 2
    refs, rest = list(rest[:sum(counts)]), rest[sum(counts):]
    local, passed, src = [
        [refs.pop(0) for _ in range(count)] for count in counts
    ]
    local, passed, src = rows_of(local), rows_of(passed), rows_of(src)
    tab_ref, w_ref = rest[:2]
    rest = rest[2:]
    if final:
        acc_ref, keep_ref, send_ref, grouped_ref, work_ref = rest
    else:
        out_ref, grouped_ref, work_ref = rest
    owns = len(local) // (NX // local[0][0].shape[1])
    count = len(src) // (NX // src[0][0].shape[1])
    halves = owns * count * NZ // LANES
    pitch = work_ref.shape[1] // NY

    low = lax.broadcasted_iota(jnp.int32, (NX, LANES), 1) < NZ
    low16 = lax.broadcasted_iota(jnp.int16, (NX, LANES), 1) < NZ

    def swapped(x):
        return jnp.concatenate([x[:, NZ:], x[:, :NZ]], 1)

    def tile(rows, j, off):
        return jnp.concatenate(
            [ref[at, :, pl.ds(off, LANES)] for ref, at in rows[j::count]], 0)

    def picked(rows, o, off):
        turn = (core + o) % owns
        return jnp.concatenate(
            [ref[at + turn, :, pl.ds(off, LANES)] for ref, at in rows[::owns]], 0)

    def own_tile(o, off):
        return jnp.where(core == chip, picked(local, o, off), picked(passed, o, off))

    def forward(t):
        at = t * QUAD * NX
        rows_d, rows_s = [], []
        for q in range(0, QUAD, LANES // NZ):
            off = (t * QUAD + q) * NZ
            a, b = tile(src, 0, off), tile(src, 1, off)
            mixed = swapped(jnp.where(low16, b, a))
            pair = [jnp.where(low16, a, mixed), jnp.where(low16, mixed, b)]
            rows_s += pair
            wide = []
            for o in range(owns):
                mine = own_tile(o, off)
                turned = swapped(mine)
                wide.append([jnp.where(low16, mine, turned), jnp.where(low16, turned, mine)])
            for y in range(2):
                rows_d.append(jnp.concatenate([w[y] * pair[y] for w in wide], 1))
        grouped_ref[pl.ds(at, QUAD * NX), :] = jnp.concatenate(rows_s, 0)
        first = product(jnp.concatenate(rows_d, 0), tab_ref[0]).astype(BF)
        modes = product(tab_ref[1], first)
        for q in range(QUAD):
            to = (t * QUAD + q) * pitch
            for h in range(halves):
                work_ref[h, pl.ds(to, NX), :] = modes[q * NX:(q + 1) * NX, h * LANES:(h + 1) * LANES]

    def solve(t):
        at = t * QUAD * NY
        modes = jnp.concatenate([
            jnp.concatenate(
                [work_ref[h, pl.ds(t * QUAD + q, NY, stride=pitch), :] for h in range(halves)], 1)
            for q in range(QUAD)], 0).astype(BF)
        weights = jnp.concatenate([w_ref[pl.ds(at, QUAD * NY), :]] * halves, 1)
        scaled = (product(tab_ref[0], modes) * weights).astype(BF)
        back = product(tab_ref[0], scaled)
        for q in range(QUAD):
            for h in range(halves):
                work_ref[h, pl.ds(t * QUAD + q, NY, stride=pitch), :] = (
                    back[q * NY:(q + 1) * NY, h * LANES:(h + 1) * LANES])

    def backward(t):
        at = t * QUAD * NX
        modes = jnp.concatenate([
            jnp.concatenate(
                [work_ref[h, pl.ds((t * QUAD + q) * pitch, NX), :] for h in range(halves)], 1)
            for q in range(QUAD)], 0).astype(BF)
        third = product(tab_ref[2], modes).astype(BF)
        potential = product(third, tab_ref[3])
        for q in range(0, QUAD, LANES // NZ):
            off = (t * QUAD + q) * NZ
            factor = [
                grouped_ref[pl.ds(at + (q + y) * NX, NX), :].astype(F32) for y in range(2)
            ]
            for o in range(owns):
                a, b = [
                    potential[(q + y) * NX:(q + y + 1) * NX, o * LANES:(o + 1) * LANES] * factor[y]
                    for y in range(2)
                ]
                exchange = jnp.where(low, a, b) + pltpu.roll(jnp.where(low, b, a), NZ, 1)
                if not final:
                    out_ref[o, :, pl.ds(off, LANES)] = exchange
                    continue
                exchange = exchange + acc_ref[o, :, pl.ds(off, LANES)]
                if o == 0:
                    keep_ref[:, pl.ds(off, LANES)] = own_tile(0, off).astype(F32) - exchange
                else:
                    send_ref[:, pl.ds(off, LANES)] = exchange.astype(send_ref.dtype)

    for step, trips in ((forward, NY // QUAD), (solve, NX // QUAD), (backward, NY // QUAD)):
        for t in range(trips):
            step(t)


def add_block(local, passed, src, tables, acc):
    owns, rows, cells = local[0].shape
    count = sum(x.shape[0] for x in src) * rows // NX
    assert count * NZ == LANES and owns == 2
    counts = (len(local), len(passed), len(src))
    final = acc is not None
    lead = () if acc is None else (acc,)
    flops = 12 * owns * count * NX * NY * NZ * NZ * 4
    if final:
        out_shape = (
            jax.ShapeDtypeStruct((NX, cells), F32), jax.ShapeDtypeStruct((NX, cells), BF))
    else:
        out_shape = jax.ShapeDtypeStruct((owns, NX, cells), F32)
    return pl.pallas_call(
        lambda *refs: block_kernel(counts, final, refs),
        out_shape=out_shape,
        in_specs=[VMEM] * (sum(counts) + 2 + len(lead)),
        out_specs=(VMEM, VMEM) if final else VMEM,
        scratch_shapes=[
            pltpu.VMEM((NY * NX, count * NZ), BF),
            pltpu.VMEM((owns * count * NZ // LANES, NY * (NX + ROW_PAD), LANES), F32),
        ],
        compiler_params=pltpu.CompilerParams(vmem_limit_bytes=24 * 1024 * 1024),
        cost_estimate=pl.CostEstimate(flops=flops, bytes_accessed=8 << 20, transcendentals=0),
    )(*local, *passed, *src, *tables, *lead)


def combine_kernel(slabs, keep_ref, part_ref, out_ref):
    grid_index = lax.axis_index("grid")
    rows = keep_ref.shape[0] // slabs
    for r in range(slabs):
        other = (r ^ 1) * rows
        updated = keep_ref[r * rows:(r + 1) * rows] - part_ref[other:other + rows].astype(F32)
        updated = updated.astype(BF)
        if len(out_ref.shape) == 3:
            out_ref[grid_index ^ r] = updated
            continue
        share = out_ref.shape[3]
        for b in range(out_ref.shape[0]):
            out_ref[b, grid_index ^ r] = updated[:, b * share:(b + 1) * share]


def gram_kernel(x_ref, out_ref):
    orbs, rows, lanes = x_ref.shape
    flat = x_ref[...].reshape(orbs * rows, lanes)
    full = lax.dot_general(flat, flat, (((1,), (1,)), ((), ())), preferred_element_type=F32)
    down = lax.broadcasted_iota(jnp.int32, (rows, orbs * rows), 0)
    along = lax.broadcasted_iota(jnp.int32, (rows, orbs * rows), 1)
    same = down == along % rows
    half = [
        jnp.sum(jnp.where(same, full[o * rows:(o + 1) * rows], 0.0), axis=0, keepdims=True)
        for o in range(orbs)
    ]
    half = jnp.concatenate(half, 0)
    gram = jnp.sum(half.T.reshape(orbs, rows, orbs), axis=1)
    deep = orbs * orbs // LANES
    packed = jnp.concatenate([gram[q * deep:(q + 1) * deep] for q in range(orbs // deep)], 1)
    out_ref[...] = jnp.broadcast_to(packed[None], out_ref.shape)


def rotate_kernel(scale, parts_ref, x_ref, out_ref, gram_ref):
    orbs, rows, lanes = x_ref.shape
    packed = jnp.sum(parts_ref[...], axis=0) * scale
    gram = jnp.concatenate(
        [packed[:, q * orbs:(q + 1) * orbs] for q in range(LANES // orbs)], 0)
    gram_ref[...] = gram
    down = lax.broadcasted_iota(jnp.int32, (orbs, orbs), 0)
    along = lax.broadcasted_iota(jnp.int32, (orbs, orbs), 1)
    eye = jnp.where(down == along, 1.0, 0.0)
    zero = jnp.zeros((orbs, LANES - 2 * orbs), F32)
    work = jnp.concatenate([gram, eye, zero], 1)
    row = lax.broadcasted_iota(jnp.int32, (orbs, LANES), 0)
    pivots = jnp.zeros((orbs, LANES), F32)
    for first in range(0, orbs, PANEL):
        columns = [
            jnp.broadcast_to(work[:, c:c + 1], (orbs, LANES)) for c in range(first, first + PANEL)
        ]
        for k in range(first, first + PANEL):
            column = columns[k - first]
            pivot = column[k:k + 1, :]
            pivots = jnp.where(row == k, pivot, pivots)
            factor = jnp.where(row > k, column * (1.0 / pivot), 0.0)
            work = work - factor * work[k:k + 1, :]
            for c in range(k - first + 1, PANEL):
                columns[c] = columns[c] - factor * columns[c][k:k + 1, :]
    work = work * (1.0 / jnp.sqrt(pivots))
    inverse = work[:, orbs:2 * orbs].astype(BF)
    tall = lax.broadcasted_iota(jnp.int32, (orbs * rows, orbs), 0) // rows
    wide = lax.broadcasted_iota(jnp.int32, (orbs * rows, orbs), 1)
    pick = jnp.where(tall == wide, 1.0, 0.0).astype(BF)
    spread = product(pick, inverse).astype(BF)
    spread = lax.dot_general(spread, pick, (((1,), (1,)), ((), ())), preferred_element_type=F32)
    i = lax.broadcasted_iota(jnp.int32, (orbs * rows, 1), 0) % rows
    j = lax.broadcasted_iota(jnp.int32, (1, orbs * rows), 1) % rows
    spread = jnp.where(i == j, spread, 0.0).astype(BF)
    flat = x_ref[...].reshape(orbs * rows, lanes)
    out_ref[...] = product(spread, flat).astype(BF).reshape(orbs, rows, lanes)


def exchanged(x, axis, by, only=None):
    return lax.ppermute(x, axis, [
        (i, i ^ by) for i in range(lax.axis_size(axis)) if only is None or only(i)])


def body(orbitals):
    orb_count, slab_rows, plane_cells = orbitals.shape
    slabs = lax.axis_size("grid")
    blocks = lax.axis_size("blk")
    assert orb_count == slabs == 4 and slab_rows * slabs == NX and blocks % 2 == 0 and STEPS == 2
    top = slabs // 2
    half = orb_count // 2
    core = lax.axis_index("grid") % 2
    even = lax.axis_index("blk") % 2 == 0
    diagonals, weights = make_tables(slab_rows)

    def shifted(x):
        return lax.ppermute(x, "blk", [(i, (i + 2) % blocks) for i in range(blocks)])

    def relayed(mine, received):
        relay = jnp.where(even, mine, received)
        return exchanged(relay, "blk", 1)

    def passed_on(x):
        return exchanged(x, "grid", 1, lambda i: i // 2 == i % 2)

    keep = lax.dynamic_slice_in_dim(orbitals, core * half, half, 0)
    give = lax.dynamic_slice_in_dim(orbitals, (1 - core) * half, half, 0)
    keep, give = lax.optimization_barrier((keep, give))
    held = [keep, exchanged(give, "grid", 1)]
    pieces = [held[0]] + list(lax.optimization_barrier(
        tuple(held[1][j:j + 1] for j in range(half))))
    far = [shifted(piece) for piece in pieces]
    across = [exchanged(held[i], "grid", top) for i in range(2)]
    near = [relayed(piece, far[i]) for i, piece in enumerate(pieces)]
    far_other = [shifted(across[0])] + [
        exchanged(far[i], "grid", top) for i in range(1, len(far))]
    relay, diagonals, weights = lax.optimization_barrier((across[0], diagonals, weights))
    tables = (diagonals, weights)
    near_other = [relayed(relay, far_other[0])] + [
        exchanged(near[i], "grid", top) for i in range(1, len(near))]
    local = held + across
    passed = [give, passed_on(held[0]), passed_on(jnp.concatenate([across[1], across[0]], 0))]
    acc = add_block(local, passed, far + far_other, tables, None)
    mine, other = add_block(local, passed, near + near_other, tables, acc)
    other = exchanged(other, "grid", 1)
    chunk = plane_cells // blocks
    if chunk % LANES == 0:
        shape = (blocks, slabs, slab_rows, chunk)
    else:
        shape = (slabs, slab_rows, plane_cells)
    updated = pl.pallas_call(
        functools.partial(combine_kernel, slabs),
        out_shape=jax.ShapeDtypeStruct(shape, BF),
        in_specs=[VMEM, VMEM],
        out_specs=VMEM,
        compiler_params=pltpu.CompilerParams(vmem_limit_bytes=SMALL_VMEM),
    )(mine, other)
    if chunk % LANES:
        updated = updated.reshape(slabs, slab_rows, blocks, chunk).transpose(2, 0, 1, 3)
    updated = updated.reshape(blocks * slabs, slab_rows, chunk)
    cellwise = lax.all_to_all(updated, ("blk", "grid"), 0, 0, tiled=True)

    devices = blocks * slabs
    cell_count = NX * NY * NZ
    if devices * slab_rows <= 512 and devices % PANEL == 0 and chunk % LANES == 0:
        local = pl.pallas_call(
            gram_kernel,
            out_shape=jax.ShapeDtypeStruct((devices, devices * devices // LANES, LANES), F32),
            in_specs=[VMEM],
            out_specs=VMEM,
            compiler_params=pltpu.CompilerParams(vmem_limit_bytes=SMALL_VMEM),
        )(cellwise)
        parts = lax.all_to_all(local, ("blk", "grid"), 0, 0, tiled=True)
        return pl.pallas_call(
            functools.partial(rotate_kernel, 1.0 / cell_count),
            out_shape=(
                jax.ShapeDtypeStruct(cellwise.shape, BF),
                jax.ShapeDtypeStruct((devices, devices), F32),
            ),
            in_specs=[VMEM, VMEM],
            out_specs=(VMEM, VMEM),
            compiler_params=pltpu.CompilerParams(vmem_limit_bytes=SMALL_VMEM),
        )(parts, cellwise)
    flat = cellwise.reshape(devices, slab_rows * chunk)
    local = jnp.dot(flat, flat.T, preferred_element_type=F32)
    intersection = lax.psum(local, ("blk", "grid")) / cell_count
    factor = jnp.linalg.cholesky(intersection)
    identity = jnp.eye(devices, dtype=F32)
    inverse = jax.scipy.linalg.solve_triangular(factor, identity, lower=True).astype(BF)
    rotated = product(inverse, flat).astype(BF)
    return (rotated.reshape(cellwise.shape), intersection)


def solution(mesh):
    in_specs = (P("blk", "grid", None),)
    out_specs = (P(None, "grid", "blk"), P())
    return jax.shard_map(body, mesh=mesh, in_specs=in_specs, out_specs=out_specs, check_vma=False)
```

```python
import functools

import jax
import jax.numpy as jnp
from jax import lax
from jax.experimental import pallas as pl
from jax.experimental.pallas import tpu as pltpu
from jax.sharding import PartitionSpec as P


NX = 64
NY = 64
NZ = 64
STEPS = 2

exchange_fraction = 0.25
screening = 1.0

BF = jnp.bfloat16
F32 = jnp.float32
VMEM = pl.BlockSpec(memory_space=pltpu.VMEM)
SMEM = pl.BlockSpec(memory_space=pltpu.SMEM)
LANES = 128
ROW_PAD = 1
SMALL_VMEM = 10 * 1024 * 1024
QUAD = 4
PANEL = 8


def product(a, b):
    return jnp.dot(a, b, preferred_element_type=F32)


def sines(rows, columns, length):
    angle = jnp.pi * (rows + 1.0) * (columns + 1.0) / (length + 1)
    return jnp.sqrt(2.0 / (length + 1)) * jnp.sin(angle)


def eigen_values(index, length):
    return 2.0 - 2.0 * jnp.cos(jnp.pi * (index + 1.0) / (length + 1))


def table_kernel(slab_rows, diag_ref, weight_ref):
    size = diag_ref.shape[1]
    copies = size // NX
    grid_index = lax.axis_index("grid")

    def cells_of(position):
        slab = position // slab_rows
        start = jnp.zeros_like(position)
        for r in range(NX // slab_rows):
            start = jnp.where(slab == r, (grid_index ^ r) * slab_rows, start)
        return start + position % slab_rows

    shape = (NX, LANES)
    down = lax.broadcasted_iota(jnp.int32, shape, 0)
    along = lax.broadcasted_iota(jnp.int32, shape, 1) % NX
    pairs = (
        (down, along),
        (down, cells_of(along)),
        (cells_of(down), along),
    )
    same = (
        lax.broadcasted_iota(jnp.int32, (NX, size), 1) // NX
    )
    for i, (row, column) in enumerate(pairs):
        table = sines(row.astype(F32), column.astype(F32), NX)
        table = jnp.concatenate([table] * (size // LANES), 1)
        for c in range(copies):
            block = jnp.where(same == c, table, 0.0).astype(BF)
            diag_ref[i, c * NX:(c + 1) * NX, :] = block
            if i == 0:
                block = (block.astype(F32) * exchange_fraction).astype(BF)
                diag_ref[len(pairs), c * NX:(c + 1) * NX, :] = block
    lam = eigen_values(down.astype(F32), NX)
    plane = screening + lam + eigen_values(along.astype(F32), NZ)
    for k in range(NX):
        weight_ref[k * NY:(k + 1) * NY, :] = 1.0 / (lam[k:k + 1, :] + plane)


def make_tables(slab_rows):
    size = QUAD * NX
    return pl.pallas_call(
        functools.partial(table_kernel, slab_rows),
        out_shape=(
            jax.ShapeDtypeStruct((4, size, size), BF),
            jax.ShapeDtypeStruct((NX * NY, LANES), F32),
        ),
        out_specs=(VMEM, VMEM),
        compiler_params=pltpu.CompilerParams(vmem_limit_bytes=SMALL_VMEM),
        cost_estimate=pl.CostEstimate(flops=1 << 28, bytes_accessed=3 << 20, transcendentals=0),
    )()


def rows_of(refs):
    return [(ref, j) for ref in refs for j in range(ref.shape[0])]


def block_kernel(counts, final, rest):
    grid_index = lax.axis_index("grid")
    core, chip = grid_index % 2, grid_index // 2
    refs, rest = list(rest[:sum(counts)]), rest[sum(counts):]
    local, passed, src = [
        [refs.pop(0) for _ in range(count)] for count in counts
    ]
    local, passed, src = rows_of(local), rows_of(passed), rows_of(src)
    tab_ref, w_ref = rest[:2]
    rest = rest[2:]
    if final:
        acc_ref, keep_ref, send_ref, grouped_ref, work_ref = rest
    else:
        out_ref, grouped_ref, work_ref = rest
    owns = len(local) // (NX // local[0][0].shape[1])
    count = len(src) // (NX // src[0][0].shape[1])
    halves = owns * count * NZ // LANES
    pitch = work_ref.shape[1] // NY

    low = lax.broadcasted_iota(jnp.int32, (NX, LANES), 1) < NZ
    low16 = lax.broadcasted_iota(jnp.int16, (NX, LANES), 1) < NZ

    def swapped(x):
        return jnp.concatenate([x[:, NZ:], x[:, :NZ]], 1)

    def tile(rows, j, off):
        return jnp.concatenate(
            [ref[at, :, pl.ds(off, LANES)] for ref, at in rows[j::count]], 0)

    def picked(rows, o, off):
        turn = (core + o) % owns
        return jnp.concatenate(
            [ref[at + turn, :, pl.ds(off, LANES)] for ref, at in rows[::owns]], 0)

    def own_tile(o, off):
        return jnp.where(core == chip, picked(local, o, off), picked(passed, o, off))

    def forward(t):
        at = t * QUAD * NX
        rows_d, rows_s = [], []
        for q in range(0, QUAD, LANES // NZ):
            off = (t * QUAD + q) * NZ
            a, b = tile(src, 0, off), tile(src, 1, off)
            mixed = swapped(jnp.where(low16, b, a))
            pair = [jnp.where(low16, a, mixed), jnp.where(low16, mixed, b)]
            rows_s += pair
            wide = []
            for o in range(owns):
                mine = own_tile(o, off)
                turned = swapped(mine)
                wide.append([jnp.where(low16, mine, turned), jnp.where(low16, turned, mine)])
            for y in range(2):
                rows_d.append(jnp.concatenate([w[y] * pair[y] for w in wide], 1))
        grouped_ref[pl.ds(at, QUAD * NX), :] = jnp.concatenate(rows_s, 0)
        first = product(jnp.concatenate(rows_d, 0), tab_ref[0]).astype(BF)
        modes = product(tab_ref[1], first)
        for q in range(QUAD):
            to = (t * QUAD + q) * pitch
            for h in range(halves):
                work_ref[h, pl.ds(to, NX), :] = modes[q * NX:(q + 1) * NX, h * LANES:(h + 1) * LANES]

    def solve(t):
        at = t * QUAD * NY
        modes = jnp.concatenate([
            jnp.concatenate(
                [work_ref[h, pl.ds(t * QUAD + q, NY, stride=pitch), :] for h in range(halves)], 1)
            for q in range(QUAD)], 0).astype(BF)
        weights = jnp.concatenate([w_ref[pl.ds(at, QUAD * NY), :]] * halves, 1)
        scaled = (product(tab_ref[0], modes) * weights).astype(BF)
        back = product(tab_ref[0], scaled)
        for q in range(QUAD):
            for h in range(halves):
                work_ref[h, pl.ds(t * QUAD + q, NY, stride=pitch), :] = (
                    back[q * NY:(q + 1) * NY, h * LANES:(h + 1) * LANES])

    def backward(t):
        at = t * QUAD * NX
        modes = jnp.concatenate([
            jnp.concatenate(
                [work_ref[h, pl.ds((t * QUAD + q) * pitch, NX), :] for h in range(halves)], 1)
            for q in range(QUAD)], 0).astype(BF)
        third = product(tab_ref[2], modes).astype(BF)
        potential = product(third, tab_ref[3])
        for q in range(0, QUAD, LANES // NZ):
            off = (t * QUAD + q) * NZ
            factor = [
                grouped_ref[pl.ds(at + (q + y) * NX, NX), :].astype(F32) for y in range(2)
            ]
            for o in range(owns):
                a, b = [
                    potential[(q + y) * NX:(q + y + 1) * NX, o * LANES:(o + 1) * LANES] * factor[y]
                    for y in range(2)
                ]
                exchange = jnp.where(low, a, b) + pltpu.roll(jnp.where(low, b, a), NZ, 1)
                if not final:
                    out_ref[o, :, pl.ds(off, LANES)] = exchange
                    continue
                exchange = exchange + acc_ref[o, :, pl.ds(off, LANES)]
                if o == 0:
                    keep_ref[:, pl.ds(off, LANES)] = own_tile(0, off).astype(F32) - exchange
                else:
                    send_ref[:, pl.ds(off, LANES)] = exchange.astype(send_ref.dtype)

    for step, trips in ((forward, NY // QUAD), (solve, NX // QUAD), (backward, NY // QUAD)):
        for t in range(trips):
            step(t)


def add_block(local, passed, src, tables, acc):
    owns, rows, cells = local[0].shape
    count = sum(x.shape[0] for x in src) * rows // NX
    assert count * NZ == LANES and owns == 2
    counts = (len(local), len(passed), len(src))
    final = acc is not None
    lead = () if acc is None else (acc,)
    flops = 12 * owns * count * NX * NY * NZ * NZ * 4
    if final:
        out_shape = (
            jax.ShapeDtypeStruct((NX, cells), F32), jax.ShapeDtypeStruct((NX, cells), BF))
    else:
        out_shape = jax.ShapeDtypeStruct((owns, NX, cells), F32)
    return pl.pallas_call(
        lambda *refs: block_kernel(counts, final, refs),
        out_shape=out_shape,
        in_specs=[VMEM] * (sum(counts) + 2 + len(lead)),
        out_specs=(VMEM, VMEM) if final else VMEM,
        scratch_shapes=[
            pltpu.VMEM((NY * NX, count * NZ), BF),
            pltpu.VMEM((owns * count * NZ // LANES, NY * (NX + ROW_PAD), LANES), F32),
        ],
        compiler_params=pltpu.CompilerParams(vmem_limit_bytes=24 * 1024 * 1024),
        cost_estimate=pl.CostEstimate(flops=flops, bytes_accessed=8 << 20, transcendentals=0),
    )(*local, *passed, *src, *tables, *lead)


def combine_kernel(slabs, keep_ref, part_ref, out_ref):
    grid_index = lax.axis_index("grid")
    rows = keep_ref.shape[0] // slabs
    for r in range(slabs):
        other = (r ^ 1) * rows
        updated = keep_ref[r * rows:(r + 1) * rows] - part_ref[other:other + rows].astype(F32)
        updated = updated.astype(BF)
        if len(out_ref.shape) == 3:
            out_ref[grid_index ^ r] = updated
            continue
        share = out_ref.shape[3]
        for b in range(out_ref.shape[0]):
            out_ref[b, grid_index ^ r] = updated[:, b * share:(b + 1) * share]


def gram_kernel(x_ref, out_ref):
    orbs, rows, lanes = x_ref.shape
    flat = x_ref[...].reshape(orbs * rows, lanes)
    full = lax.dot_general(flat, flat, (((1,), (1,)), ((), ())), preferred_element_type=F32)
    down = lax.broadcasted_iota(jnp.int32, (rows, orbs * rows), 0)
    along = lax.broadcasted_iota(jnp.int32, (rows, orbs * rows), 1)
    same = down == along % rows
    half = [
        jnp.sum(jnp.where(same, full[o * rows:(o + 1) * rows], 0.0), axis=0, keepdims=True)
        for o in range(orbs)
    ]
    half = jnp.concatenate(half, 0)
    gram = jnp.sum(half.T.reshape(orbs, rows, orbs), axis=1)
    deep = orbs * orbs // LANES
    packed = jnp.concatenate([gram[q * deep:(q + 1) * deep] for q in range(orbs // deep)], 1)
    out_ref[...] = jnp.broadcast_to(packed[None], out_ref.shape)


def rotate_kernel(scale, parts_ref, x_ref, out_ref, gram_ref):
    orbs, rows, lanes = x_ref.shape
    packed = jnp.sum(parts_ref[...], axis=0) * scale
    gram = jnp.concatenate(
        [packed[:, q * orbs:(q + 1) * orbs] for q in range(LANES // orbs)], 0)
    gram_ref[...] = gram
    down = lax.broadcasted_iota(jnp.int32, (orbs, orbs), 0)
    along = lax.broadcasted_iota(jnp.int32, (orbs, orbs), 1)
    eye = jnp.where(down == along, 1.0, 0.0)
    zero = jnp.zeros((orbs, LANES - 2 * orbs), F32)
    work = jnp.concatenate([gram, eye, zero], 1)
    row = lax.broadcasted_iota(jnp.int32, (orbs, LANES), 0)
    pivots = jnp.zeros((orbs, LANES), F32)
    for first in range(0, orbs, PANEL):
        columns = [
            jnp.broadcast_to(work[:, c:c + 1], (orbs, LANES)) for c in range(first, first + PANEL)
        ]
        for k in range(first, first + PANEL):
            column = columns[k - first]
            pivot = column[k:k + 1, :]
            pivots = jnp.where(row == k, pivot, pivots)
            factor = jnp.where(row > k, column * (1.0 / pivot), 0.0)
            work = work - factor * work[k:k + 1, :]
            for c in range(k - first + 1, PANEL):
                columns[c] = columns[c] - factor * columns[c][k:k + 1, :]
    work = work * (1.0 / jnp.sqrt(pivots))
    inverse = work[:, orbs:2 * orbs].astype(BF)
    tall = lax.broadcasted_iota(jnp.int32, (orbs * rows, orbs), 0) // rows
    wide = lax.broadcasted_iota(jnp.int32, (orbs * rows, orbs), 1)
    pick = jnp.where(tall == wide, 1.0, 0.0).astype(BF)
    spread = product(pick, inverse).astype(BF)
    spread = lax.dot_general(spread, pick, (((1,), (1,)), ((), ())), preferred_element_type=F32)
    i = lax.broadcasted_iota(jnp.int32, (orbs * rows, 1), 0) % rows
    j = lax.broadcasted_iota(jnp.int32, (1, orbs * rows), 1) % rows
    spread = jnp.where(i == j, spread, 0.0).astype(BF)
    flat = x_ref[...].reshape(orbs * rows, lanes)
    out_ref[...] = product(spread, flat).astype(BF).reshape(orbs, rows, lanes)


def exchanged(x, axis, by, only=None):
    return lax.ppermute(x, axis, [
        (i, i ^ by) for i in range(lax.axis_size(axis)) if only is None or only(i)])


def body(orbitals):
    orb_count, slab_rows, plane_cells = orbitals.shape
    slabs = lax.axis_size("grid")
    blocks = lax.axis_size("blk")
    assert orb_count == slabs == 4 and slab_rows * slabs == NX and blocks % 2 == 0 and STEPS == 2
    top = slabs // 2
    half = orb_count // 2
    core = lax.axis_index("grid") % 2
    even = lax.axis_index("blk") % 2 == 0
    diagonals, weights = make_tables(slab_rows)

    def shifted(x):
        return lax.ppermute(x, "blk", [(i, (i + 2) % blocks) for i in range(blocks)])

    def relayed(mine, received):
        relay = jnp.where(even, mine, received)
        return exchanged(relay, "blk", 1)

    def passed_on(x):
        return exchanged(x, "grid", 1, lambda i: i // 2 == i % 2)

    keep = lax.dynamic_slice_in_dim(orbitals, core * half, half, 0)
    give = lax.dynamic_slice_in_dim(orbitals, (1 - core) * half, half, 0)
    keep, give = lax.optimization_barrier((keep, give))
    held = [keep, exchanged(give, "grid", 1)]
    far = [shifted(held[i]) for i in range(2)]
    across = [exchanged(held[i], "grid", top) for i in range(2)]
    near = [relayed(held[i], far[i]) for i in range(2)]
    far_other = [exchanged(far[0], "grid", top), shifted(across[1])]
    relay, diagonals, weights = lax.optimization_barrier((across[1], diagonals, weights))
    tables = (diagonals, weights)
    near_other = [exchanged(near[0], "grid", top), relayed(relay, far_other[1])]
    local = held + across
    passed = [give, passed_on(held[0]), passed_on(jnp.concatenate([across[1], across[0]], 0))]
    acc = add_block(local, passed, far + far_other, tables, None)
    mine, other = add_block(local, passed, near + near_other, tables, acc)
    other = exchanged(other, "grid", 1)
    chunk = plane_cells // blocks
    if chunk % LANES == 0:
        shape = (blocks, slabs, slab_rows, chunk)
    else:
        shape = (slabs, slab_rows, plane_cells)
    updated = pl.pallas_call(
        functools.partial(combine_kernel, slabs),
        out_shape=jax.ShapeDtypeStruct(shape, BF),
        in_specs=[VMEM, VMEM],
        out_specs=VMEM,
        compiler_params=pltpu.CompilerParams(vmem_limit_bytes=SMALL_VMEM),
    )(mine, other)
    if chunk % LANES:
        updated = updated.reshape(slabs, slab_rows, blocks, chunk).transpose(2, 0, 1, 3)
    updated = updated.reshape(blocks * slabs, slab_rows, chunk)
    cellwise = lax.all_to_all(updated, ("blk", "grid"), 0, 0, tiled=True)

    devices = blocks * slabs
    cell_count = NX * NY * NZ
    if devices * slab_rows <= 512 and devices % PANEL == 0 and chunk % LANES == 0:
        local = pl.pallas_call(
            gram_kernel,
            out_shape=jax.ShapeDtypeStruct((devices, devices * devices // LANES, LANES), F32),
            in_specs=[VMEM],
            out_specs=VMEM,
            compiler_params=pltpu.CompilerParams(vmem_limit_bytes=SMALL_VMEM),
        )(cellwise)
        parts = lax.all_to_all(local, ("blk", "grid"), 0, 0, tiled=True)
        return pl.pallas_call(
            functools.partial(rotate_kernel, 1.0 / cell_count),
            out_shape=(
                jax.ShapeDtypeStruct(cellwise.shape, BF),
                jax.ShapeDtypeStruct((devices, devices), F32),
            ),
            in_specs=[VMEM, VMEM],
            out_specs=(VMEM, VMEM),
            compiler_params=pltpu.CompilerParams(vmem_limit_bytes=SMALL_VMEM),
        )(parts, cellwise)
    flat = cellwise.reshape(devices, slab_rows * chunk)
    local = jnp.dot(flat, flat.T, preferred_element_type=F32)
    intersection = lax.psum(local, ("blk", "grid")) / cell_count
    factor = jnp.linalg.cholesky(intersection)
    identity = jnp.eye(devices, dtype=F32)
    inverse = jax.scipy.linalg.solve_triangular(factor, identity, lower=True).astype(BF)
    rotated = product(inverse, flat).astype(BF)
    return (rotated.reshape(cellwise.shape), intersection)


def solution(mesh):
    in_specs = (P("blk", "grid", None),)
    out_specs = (P(None, "grid", "blk"), P())
    return jax.shard_map(body, mesh=mesh, in_specs=in_specs, out_specs=out_specs, check_vma=False)
```

```python
import functools

import jax
import jax.numpy as jnp
from jax import lax
from jax.experimental import pallas as pl
from jax.experimental.pallas import tpu as pltpu
from jax.sharding import PartitionSpec as P


NX = 64
NY = 64
NZ = 64
STEPS = 2

exchange_fraction = 0.25
screening = 1.0

BF = jnp.bfloat16
F32 = jnp.float32
VMEM = pl.BlockSpec(memory_space=pltpu.VMEM)
SMEM = pl.BlockSpec(memory_space=pltpu.SMEM)
LANES = 128
ROW_PAD = 1
SMALL_VMEM = 10 * 1024 * 1024
QUAD = 4
PANEL = 8


def product(a, b):
    return jnp.dot(a, b, preferred_element_type=F32)


def sines(rows, columns, length):
    angle = jnp.pi * (rows + 1.0) * (columns + 1.0) / (length + 1)
    return jnp.sqrt(2.0 / (length + 1)) * jnp.sin(angle)


def eigen_values(index, length):
    return 2.0 - 2.0 * jnp.cos(jnp.pi * (index + 1.0) / (length + 1))


def table_kernel(slab_rows, diag_ref, weight_ref):
    size = diag_ref.shape[1]
    copies = size // NX
    grid_index = lax.axis_index("grid")

    def cells_of(position):
        slab = position // slab_rows
        start = jnp.zeros_like(position)
        for r in range(NX // slab_rows):
            start = jnp.where(slab == r, (grid_index ^ r) * slab_rows, start)
        return start + position % slab_rows

    shape = (NX, LANES)
    down = lax.broadcasted_iota(jnp.int32, shape, 0)
    along = lax.broadcasted_iota(jnp.int32, shape, 1) % NX
    pairs = (
        (down, along),
        (down, cells_of(along)),
        (cells_of(down), along),
    )
    same = (
        lax.broadcasted_iota(jnp.int32, (NX, size), 1) // NX
    )
    for i, (row, column) in enumerate(pairs):
        table = sines(row.astype(F32), column.astype(F32), NX)
        table = jnp.concatenate([table] * (size // LANES), 1)
        for c in range(copies):
            block = jnp.where(same == c, table, 0.0).astype(BF)
            diag_ref[i, c * NX:(c + 1) * NX, :] = block
            if i == 0:
                block = (block.astype(F32) * exchange_fraction).astype(BF)
                diag_ref[len(pairs), c * NX:(c + 1) * NX, :] = block
    lam = eigen_values(down.astype(F32), NX)
    plane = screening + lam + eigen_values(along.astype(F32), NZ)
    for k in range(NX):
        weight_ref[k * NY:(k + 1) * NY, :] = 1.0 / (lam[k:k + 1, :] + plane)


def make_tables(slab_rows):
    size = QUAD * NX
    return pl.pallas_call(
        functools.partial(table_kernel, slab_rows),
        out_shape=(
            jax.ShapeDtypeStruct((4, size, size), BF),
            jax.ShapeDtypeStruct((NX * NY, LANES), F32),
        ),
        out_specs=(VMEM, VMEM),
        compiler_params=pltpu.CompilerParams(vmem_limit_bytes=SMALL_VMEM),
        cost_estimate=pl.CostEstimate(flops=1 << 28, bytes_accessed=3 << 20, transcendentals=0),
    )()


def rows_of(refs):
    return [(ref, j) for ref in refs for j in range(ref.shape[0])]


def block_kernel(counts, final, rest):
    grid_index = lax.axis_index("grid")
    core, chip = grid_index % 2, grid_index // 2
    refs, rest = list(rest[:sum(counts)]), rest[sum(counts):]
    local, passed, src = [
        [refs.pop(0) for _ in range(count)] for count in counts
    ]
    local, passed, src = rows_of(local), rows_of(passed), rows_of(src)
    tab_ref, w_ref = rest[:2]
    rest = rest[2:]
    if final:
        acc_ref, keep_ref, send_ref, grouped_ref, work_ref = rest
    else:
        out_ref, grouped_ref, work_ref = rest
    owns = len(local) // (NX // local[0][0].shape[1])
    count = len(src) // (NX // src[0][0].shape[1])
    halves = owns * count * NZ // LANES
    pitch = work_ref.shape[1] // NY

    low = lax.broadcasted_iota(jnp.int32, (NX, LANES), 1) < NZ
    low16 = lax.broadcasted_iota(jnp.int16, (NX, LANES), 1) < NZ

    def swapped(x):
        return jnp.concatenate([x[:, NZ:], x[:, :NZ]], 1)

    def tile(rows, j, off):
        return jnp.concatenate(
            [ref[at, :, pl.ds(off, LANES)] for ref, at in rows[j::count]], 0)

    def picked(rows, o, off):
        turn = (core + o) % owns
        return jnp.concatenate(
            [ref[at + turn, :, pl.ds(off, LANES)] for ref, at in rows[::owns]], 0)

    def own_tile(o, off):
        return jnp.where(core == chip, picked(local, o, off), picked(passed, o, off))

    def forward(t):
        at = t * QUAD * NX
        rows_d, rows_s = [], []
        for q in range(0, QUAD, LANES // NZ):
            off = (t * QUAD + q) * NZ
            a, b = tile(src, 0, off), tile(src, 1, off)
            mixed = swapped(jnp.where(low16, b, a))
            pair = [jnp.where(low16, a, mixed), jnp.where(low16, mixed, b)]
            rows_s += pair
            wide = []
            for o in range(owns):
                mine = own_tile(o, off)
                turned = swapped(mine)
                wide.append([jnp.where(low16, mine, turned), jnp.where(low16, turned, mine)])
            for y in range(2):
                rows_d.append(jnp.concatenate([w[y] * pair[y] for w in wide], 1))
        grouped_ref[pl.ds(at, QUAD * NX), :] = jnp.concatenate(rows_s, 0)
        first = product(jnp.concatenate(rows_d, 0), tab_ref[0]).astype(BF)
        modes = product(tab_ref[1], first)
        for q in range(QUAD):
            to = (t * QUAD + q) * pitch
            for h in range(halves):
                work_ref[h, pl.ds(to, NX), :] = modes[q * NX:(q + 1) * NX, h * LANES:(h + 1) * LANES]

    def solve(t):
        at = t * QUAD * NY
        modes = jnp.concatenate([
            jnp.concatenate(
                [work_ref[h, pl.ds(t * QUAD + q, NY, stride=pitch), :] for h in range(halves)], 1)
            for q in range(QUAD)], 0).astype(BF)
        weights = jnp.concatenate([w_ref[pl.ds(at, QUAD * NY), :]] * halves, 1)
        scaled = (product(tab_ref[0], modes) * weights).astype(BF)
        back = product(tab_ref[0], scaled)
        for q in range(QUAD):
            for h in range(halves):
                work_ref[h, pl.ds(t * QUAD + q, NY, stride=pitch), :] = (
                    back[q * NY:(q + 1) * NY, h * LANES:(h + 1) * LANES])

    def backward(t):
        at = t * QUAD * NX
        modes = jnp.concatenate([
            jnp.concatenate(
                [work_ref[h, pl.ds((t * QUAD + q) * pitch, NX), :] for h in range(halves)], 1)
            for q in range(QUAD)], 0).astype(BF)
        third = product(tab_ref[2], modes).astype(BF)
        potential = product(third, tab_ref[3])
        for q in range(0, QUAD, LANES // NZ):
            off = (t * QUAD + q) * NZ
            factor = [
                grouped_ref[pl.ds(at + (q + y) * NX, NX), :].astype(F32) for y in range(2)
            ]
            for o in range(owns):
                a, b = [
                    potential[(q + y) * NX:(q + y + 1) * NX, o * LANES:(o + 1) * LANES] * factor[y]
                    for y in range(2)
                ]
                exchange = jnp.where(low, a, b) + pltpu.roll(jnp.where(low, b, a), NZ, 1)
                if not final:
                    out_ref[o, :, pl.ds(off, LANES)] = exchange
                    continue
                exchange = exchange + acc_ref[o, :, pl.ds(off, LANES)]
                if o == 0:
                    keep_ref[:, pl.ds(off, LANES)] = own_tile(0, off).astype(F32) - exchange
                else:
                    send_ref[:, pl.ds(off, LANES)] = exchange.astype(send_ref.dtype)

    for step, trips in ((forward, NY // QUAD), (solve, NX // QUAD), (backward, NY // QUAD)):
        for t in range(trips):
            step(t)


def add_block(local, passed, src, tables, acc):
    owns, rows, cells = local[0].shape
    count = sum(x.shape[0] for x in src) * rows // NX
    assert count * NZ == LANES and owns == 2
    counts = (len(local), len(passed), len(src))
    final = acc is not None
    lead = () if acc is None else (acc,)
    flops = 12 * owns * count * NX * NY * NZ * NZ * 4
    if final:
        out_shape = (
            jax.ShapeDtypeStruct((NX, cells), F32), jax.ShapeDtypeStruct((NX, cells), BF))
    else:
        out_shape = jax.ShapeDtypeStruct((owns, NX, cells), F32)
    return pl.pallas_call(
        lambda *refs: block_kernel(counts, final, refs),
        out_shape=out_shape,
        in_specs=[VMEM] * (sum(counts) + 2 + len(lead)),
        out_specs=(VMEM, VMEM) if final else VMEM,
        scratch_shapes=[
            pltpu.VMEM((NY * NX, count * NZ), BF),
            pltpu.VMEM((owns * count * NZ // LANES, NY * (NX + ROW_PAD), LANES), F32),
        ],
        compiler_params=pltpu.CompilerParams(vmem_limit_bytes=24 * 1024 * 1024),
        cost_estimate=pl.CostEstimate(flops=flops, bytes_accessed=8 << 20, transcendentals=0),
    )(*local, *passed, *src, *tables, *lead)


def combine_kernel(slabs, keep_ref, part_ref, out_ref):
    grid_index = lax.axis_index("grid")
    rows = keep_ref.shape[0] // slabs
    for r in range(slabs):
        other = (r ^ 1) * rows
        updated = keep_ref[r * rows:(r + 1) * rows] - part_ref[other:other + rows].astype(F32)
        updated = updated.astype(BF)
        if len(out_ref.shape) == 3:
            out_ref[grid_index ^ r] = updated
            continue
        share = out_ref.shape[3]
        for b in range(out_ref.shape[0]):
            out_ref[b, grid_index ^ r] = updated[:, b * share:(b + 1) * share]


def gram_kernel(x_ref, out_ref):
    orbs, rows, lanes = x_ref.shape
    flat = x_ref[...].reshape(orbs * rows, lanes)
    full = lax.dot_general(flat, flat, (((1,), (1,)), ((), ())), preferred_element_type=F32)
    down = lax.broadcasted_iota(jnp.int32, (rows, orbs * rows), 0)
    along = lax.broadcasted_iota(jnp.int32, (rows, orbs * rows), 1)
    same = down == along % rows
    half = [
        jnp.sum(jnp.where(same, full[o * rows:(o + 1) * rows], 0.0), axis=0, keepdims=True)
        for o in range(orbs)
    ]
    half = jnp.concatenate(half, 0)
    gram = jnp.sum(half.T.reshape(orbs, rows, orbs), axis=1)
    deep = orbs * orbs // LANES
    packed = jnp.concatenate([gram[q * deep:(q + 1) * deep] for q in range(orbs // deep)], 1)
    out_ref[...] = jnp.broadcast_to(packed[None], out_ref.shape)


def rotate_kernel(scale, parts_ref, x_ref, out_ref, gram_ref):
    orbs, rows, lanes = x_ref.shape
    packed = jnp.sum(parts_ref[...], axis=0) * scale
    gram = jnp.concatenate(
        [packed[:, q * orbs:(q + 1) * orbs] for q in range(LANES // orbs)], 0)
    gram_ref[...] = gram
    down = lax.broadcasted_iota(jnp.int32, (orbs, orbs), 0)
    along = lax.broadcasted_iota(jnp.int32, (orbs, orbs), 1)
    eye = jnp.where(down == along, 1.0, 0.0)
    zero = jnp.zeros((orbs, LANES - 2 * orbs), F32)
    work = jnp.concatenate([gram, eye, zero], 1)
    row = lax.broadcasted_iota(jnp.int32, (orbs, LANES), 0)
    pivots = jnp.zeros((orbs, LANES), F32)
    for first in range(0, orbs, PANEL):
        columns = [
            jnp.broadcast_to(work[:, c:c + 1], (orbs, LANES)) for c in range(first, first + PANEL)
        ]
        for k in range(first, first + PANEL):
            column = columns[k - first]
            pivot = column[k:k + 1, :]
            pivots = jnp.where(row == k, pivot, pivots)
            factor = jnp.where(row > k, column * (1.0 / pivot), 0.0)
            work = work - factor * work[k:k + 1, :]
            for c in range(k - first + 1, PANEL):
                columns[c] = columns[c] - factor * columns[c][k:k + 1, :]
    work = work * (1.0 / jnp.sqrt(pivots))
    inverse = work[:, orbs:2 * orbs].astype(BF)
    tall = lax.broadcasted_iota(jnp.int32, (orbs * rows, orbs), 0) // rows
    wide = lax.broadcasted_iota(jnp.int32, (orbs * rows, orbs), 1)
    pick = jnp.where(tall == wide, 1.0, 0.0).astype(BF)
    spread = product(pick, inverse).astype(BF)
    spread = lax.dot_general(spread, pick, (((1,), (1,)), ((), ())), preferred_element_type=F32)
    i = lax.broadcasted_iota(jnp.int32, (orbs * rows, 1), 0) % rows
    j = lax.broadcasted_iota(jnp.int32, (1, orbs * rows), 1) % rows
    spread = jnp.where(i == j, spread, 0.0).astype(BF)
    flat = x_ref[...].reshape(orbs * rows, lanes)
    out_ref[...] = product(spread, flat).astype(BF).reshape(orbs, rows, lanes)


def exchanged(x, axis, by, only=None):
    return lax.ppermute(x, axis, [
        (i, i ^ by) for i in range(lax.axis_size(axis)) if only is None or only(i)])


def body(orbitals):
    orb_count, slab_rows, plane_cells = orbitals.shape
    slabs = lax.axis_size("grid")
    blocks = lax.axis_size("blk")
    assert orb_count == slabs == 4 and slab_rows * slabs == NX and blocks % 2 == 0 and STEPS == 2
    top = slabs // 2
    half = orb_count // 2
    core = lax.axis_index("grid") % 2
    even = lax.axis_index("blk") % 2 == 0
    diagonals, weights = make_tables(slab_rows)

    def shifted(x):
        return lax.ppermute(x, "blk", [(i, (i + 2) % blocks) for i in range(blocks)])

    def relayed(mine, received):
        relay = jnp.where(even, mine, received)
        return exchanged(relay, "blk", 1)

    def passed_on(x):
        return exchanged(x, "grid", 1, lambda i: i // 2 == i % 2)

    keep = lax.dynamic_slice_in_dim(orbitals, core * half, half, 0)
    give = lax.dynamic_slice_in_dim(orbitals, (1 - core) * half, half, 0)
    keep, give = lax.optimization_barrier((keep, give))
    held = [keep, exchanged(give, "grid", 1)]
    far = [shifted(held[i]) for i in range(2)]
    across = [
        exchanged(held[0], "grid", top, lambda i: i // 2 != i % 2), exchanged(held[1], "grid", top)
    ]
    near = [relayed(held[i], far[i]) for i in range(2)]
    far_other = [exchanged(far[0], "grid", top), shifted(across[1])]
    relay, diagonals, weights = lax.optimization_barrier((across[1], diagonals, weights))
    tables = (diagonals, weights)
    near_other = [exchanged(near[0], "grid", top), relayed(relay, far_other[1])]
    local = held + across
    joined = jnp.concatenate([across[1], across[0]], 0)
    passed = [give, passed_on(held[0]), passed_on(joined)]
    acc = add_block(local, passed, far + far_other, tables, None)
    mine, other = add_block(local, passed, near + near_other, tables, acc)
    other = exchanged(other, "grid", 1)
    chunk = plane_cells // blocks
    if chunk % LANES == 0:
        shape = (blocks, slabs, slab_rows, chunk)
    else:
        shape = (slabs, slab_rows, plane_cells)
    updated = pl.pallas_call(
        functools.partial(combine_kernel, slabs),
        out_shape=jax.ShapeDtypeStruct(shape, BF),
        in_specs=[VMEM, VMEM],
        out_specs=VMEM,
        compiler_params=pltpu.CompilerParams(vmem_limit_bytes=SMALL_VMEM),
    )(mine, other)
    if chunk % LANES:
        updated = updated.reshape(slabs, slab_rows, blocks, chunk).transpose(2, 0, 1, 3)
    updated = updated.reshape(blocks * slabs, slab_rows, chunk)
    cellwise = lax.all_to_all(updated, ("blk", "grid"), 0, 0, tiled=True)

    devices = blocks * slabs
    cell_count = NX * NY * NZ
    if devices * slab_rows <= 512 and devices % PANEL == 0 and chunk % LANES == 0:
        local = pl.pallas_call(
            gram_kernel,
            out_shape=jax.ShapeDtypeStruct((devices, devices * devices // LANES, LANES), F32),
            in_specs=[VMEM],
            out_specs=VMEM,
            compiler_params=pltpu.CompilerParams(vmem_limit_bytes=SMALL_VMEM),
        )(cellwise)
        parts = lax.all_to_all(local, ("blk", "grid"), 0, 0, tiled=True)
        return pl.pallas_call(
            functools.partial(rotate_kernel, 1.0 / cell_count),
            out_shape=(
                jax.ShapeDtypeStruct(cellwise.shape, BF),
                jax.ShapeDtypeStruct((devices, devices), F32),
            ),
            in_specs=[VMEM, VMEM],
            out_specs=(VMEM, VMEM),
            compiler_params=pltpu.CompilerParams(vmem_limit_bytes=SMALL_VMEM),
        )(parts, cellwise)
    flat = cellwise.reshape(devices, slab_rows * chunk)
    local = jnp.dot(flat, flat.T, preferred_element_type=F32)
    intersection = lax.psum(local, ("blk", "grid")) / cell_count
    factor = jnp.linalg.cholesky(intersection)
    identity = jnp.eye(devices, dtype=F32)
    inverse = jax.scipy.linalg.solve_triangular(factor, identity, lower=True).astype(BF)
    rotated = product(inverse, flat).astype(BF)
    return (rotated.reshape(cellwise.shape), intersection)


def solution(mesh):
    in_specs = (P("blk", "grid", None),)
    out_specs = (P(None, "grid", "blk"), P())
    return jax.shard_map(body, mesh=mesh, in_specs=in_specs, out_specs=out_specs, check_vma=False)
```

```python
import functools

import jax
import jax.numpy as jnp
from jax import lax
from jax.experimental import pallas as pl
from jax.experimental.pallas import tpu as pltpu
from jax.sharding import PartitionSpec as P


NX = 64
NY = 64
NZ = 64
STEPS = 2

exchange_fraction = 0.25
screening = 1.0

BF = jnp.bfloat16
F32 = jnp.float32
VMEM = pl.BlockSpec(memory_space=pltpu.VMEM)
SMEM = pl.BlockSpec(memory_space=pltpu.SMEM)
LANES = 128
ROW_PAD = 1
SMALL_VMEM = 10 * 1024 * 1024
QUAD = 4
PANEL = 4


def product(a, b):
    return jnp.dot(a, b, preferred_element_type=F32)


def sines(rows, columns, length):
    angle = jnp.pi * (rows + 1.0) * (columns + 1.0) / (length + 1)
    return jnp.sqrt(2.0 / (length + 1)) * jnp.sin(angle)


def eigen_values(index, length):
    return 2.0 - 2.0 * jnp.cos(jnp.pi * (index + 1.0) / (length + 1))


def table_kernel(slab_rows, diag_ref, weight_ref):
    size = diag_ref.shape[1]
    copies = size // NX
    grid_index = lax.axis_index("grid")

    def cells_of(position):
        slab = position // slab_rows
        start = jnp.zeros_like(position)
        for r in range(NX // slab_rows):
            start = jnp.where(slab == r, (grid_index ^ r) * slab_rows, start)
        return start + position % slab_rows

    shape = (NX, LANES)
    down = lax.broadcasted_iota(jnp.int32, shape, 0)
    along = lax.broadcasted_iota(jnp.int32, shape, 1) % NX
    pairs = (
        (down, along),
        (down, cells_of(along)),
        (cells_of(down), along),
    )
    same = (
        lax.broadcasted_iota(jnp.int32, (NX, size), 1) // NX
    )
    for i, (row, column) in enumerate(pairs):
        table = sines(row.astype(F32), column.astype(F32), NX)
        table = jnp.concatenate([table] * (size // LANES), 1)
        for c in range(copies):
            block = jnp.where(same == c, table, 0.0).astype(BF)
            diag_ref[i, c * NX:(c + 1) * NX, :] = block
            if i == 0:
                block = (block.astype(F32) * exchange_fraction).astype(BF)
                diag_ref[len(pairs), c * NX:(c + 1) * NX, :] = block
    lam = eigen_values(down.astype(F32), NX)
    plane = screening + lam + eigen_values(along.astype(F32), NZ)
    for k in range(NX):
        weight_ref[k * NY:(k + 1) * NY, :] = 1.0 / (lam[k:k + 1, :] + plane)


def make_tables(slab_rows):
    size = QUAD * NX
    return pl.pallas_call(
        functools.partial(table_kernel, slab_rows),
        out_shape=(
            jax.ShapeDtypeStruct((4, size, size), BF),
            jax.ShapeDtypeStruct((NX * NY, LANES), F32),
        ),
        out_specs=(VMEM, VMEM),
        compiler_params=pltpu.CompilerParams(vmem_limit_bytes=SMALL_VMEM),
        cost_estimate=pl.CostEstimate(flops=1 << 28, bytes_accessed=3 << 20, transcendentals=0),
    )()


def rows_of(refs):
    return [(ref, j) for ref in refs for j in range(ref.shape[0])]


def block_kernel(counts, final, rest):
    grid_index = lax.axis_index("grid")
    core, chip = grid_index % 2, grid_index // 2
    refs, rest = list(rest[:sum(counts)]), rest[sum(counts):]
    local, passed, src = [
        [refs.pop(0) for _ in range(count)] for count in counts
    ]
    local, passed, src = rows_of(local), rows_of(passed), rows_of(src)
    tab_ref, w_ref = rest[:2]
    rest = rest[2:]
    if final:
        acc_ref, keep_ref, send_ref, grouped_ref, work_ref = rest
    else:
        out_ref, grouped_ref, work_ref = rest
    owns = len(local) // (NX // local[0][0].shape[1])
    count = len(src) // (NX // src[0][0].shape[1])
    halves = owns * count * NZ // LANES
    pitch = work_ref.shape[1] // NY

    low = lax.broadcasted_iota(jnp.int32, (NX, LANES), 1) < NZ
    low16 = lax.broadcasted_iota(jnp.int16, (NX, LANES), 1) < NZ

    def swapped(x):
        return jnp.concatenate([x[:, NZ:], x[:, :NZ]], 1)

    def tile(rows, j, off):
        return jnp.concatenate(
            [ref[at, :, pl.ds(off, LANES)] for ref, at in rows[j::count]], 0)

    def picked(rows, o, off):
        turn = (core + o) % owns
        return jnp.concatenate(
            [ref[at + turn, :, pl.ds(off, LANES)] for ref, at in rows[::owns]], 0)

    def own_tile(o, off):
        return jnp.where(core == chip, picked(local, o, off), picked(passed, o, off))

    def forward(t):
        at = t * QUAD * NX
        rows_d, rows_s = [], []
        for q in range(0, QUAD, LANES // NZ):
            off = (t * QUAD + q) * NZ
            a, b = tile(src, 0, off), tile(src, 1, off)
            mixed = swapped(jnp.where(low16, b, a))
            pair = [jnp.where(low16, a, mixed), jnp.where(low16, mixed, b)]
            rows_s += pair
            wide = []
            for o in range(owns):
                mine = own_tile(o, off)
                turned = swapped(mine)
                wide.append([jnp.where(low16, mine, turned), jnp.where(low16, turned, mine)])
            for y in range(2):
                rows_d.append(jnp.concatenate([w[y] * pair[y] for w in wide], 1))
        grouped_ref[pl.ds(at, QUAD * NX), :] = jnp.concatenate(rows_s, 0)
        first = product(jnp.concatenate(rows_d, 0), tab_ref[0]).astype(BF)
        modes = product(tab_ref[1], first)
        for q in range(QUAD):
            to = (t * QUAD + q) * pitch
            for h in range(halves):
                work_ref[h, pl.ds(to, NX), :] = modes[q * NX:(q + 1) * NX, h * LANES:(h + 1) * LANES]

    def solve(t):
        at = t * QUAD * NY
        modes = jnp.concatenate([
            jnp.concatenate(
                [work_ref[h, pl.ds(t * QUAD + q, NY, stride=pitch), :] for h in range(halves)], 1)
            for q in range(QUAD)], 0).astype(BF)
        weights = jnp.concatenate([w_ref[pl.ds(at, QUAD * NY), :]] * halves, 1)
        scaled = (product(tab_ref[0], modes) * weights).astype(BF)
        back = product(tab_ref[0], scaled)
        for q in range(QUAD):
            for h in range(halves):
                work_ref[h, pl.ds(t * QUAD + q, NY, stride=pitch), :] = (
                    back[q * NY:(q + 1) * NY, h * LANES:(h + 1) * LANES])

    def backward(t):
        at = t * QUAD * NX
        modes = jnp.concatenate([
            jnp.concatenate(
                [work_ref[h, pl.ds((t * QUAD + q) * pitch, NX), :] for h in range(halves)], 1)
            for q in range(QUAD)], 0).astype(BF)
        third = product(tab_ref[2], modes).astype(BF)
        potential = product(third, tab_ref[3])
        for q in range(0, QUAD, LANES // NZ):
            off = (t * QUAD + q) * NZ
            factor = [
                grouped_ref[pl.ds(at + (q + y) * NX, NX), :].astype(F32) for y in range(2)
            ]
            for o in range(owns):
                a, b = [
                    potential[(q + y) * NX:(q + y + 1) * NX, o * LANES:(o + 1) * LANES] * factor[y]
                    for y in range(2)
                ]
                exchange = jnp.where(low, a, b) + pltpu.roll(jnp.where(low, b, a), NZ, 1)
                if not final:
                    out_ref[o, :, pl.ds(off, LANES)] = exchange
                    continue
                exchange = exchange + acc_ref[o, :, pl.ds(off, LANES)]
                if o == 0:
                    keep_ref[:, pl.ds(off, LANES)] = own_tile(0, off).astype(F32) - exchange
                else:
                    send_ref[:, pl.ds(off, LANES)] = exchange.astype(send_ref.dtype)

    for step, trips in ((forward, NY // QUAD), (solve, NX // QUAD), (backward, NY // QUAD)):
        for t in range(trips):
            step(t)


def add_block(local, passed, src, tables, acc):
    owns, rows, cells = local[0].shape
    count = sum(x.shape[0] for x in src) * rows // NX
    assert count * NZ == LANES and owns == 2
    counts = (len(local), len(passed), len(src))
    final = acc is not None
    lead = () if acc is None else (acc,)
    flops = 12 * owns * count * NX * NY * NZ * NZ * 4
    if final:
        out_shape = (
            jax.ShapeDtypeStruct((NX, cells), F32), jax.ShapeDtypeStruct((NX, cells), BF))
    else:
        out_shape = jax.ShapeDtypeStruct((owns, NX, cells), F32)
    return pl.pallas_call(
        lambda *refs: block_kernel(counts, final, refs),
        out_shape=out_shape,
        in_specs=[VMEM] * (sum(counts) + 2 + len(lead)),
        out_specs=(VMEM, VMEM) if final else VMEM,
        scratch_shapes=[
            pltpu.VMEM((NY * NX, count * NZ), BF),
            pltpu.VMEM((owns * count * NZ // LANES, NY * (NX + ROW_PAD), LANES), F32),
        ],
        compiler_params=pltpu.CompilerParams(vmem_limit_bytes=24 * 1024 * 1024),
        cost_estimate=pl.CostEstimate(flops=flops, bytes_accessed=8 << 20, transcendentals=0),
    )(*local, *passed, *src, *tables, *lead)


def combine_kernel(slabs, keep_ref, part_ref, out_ref):
    grid_index = lax.axis_index("grid")
    rows = keep_ref.shape[0] // slabs
    for r in range(slabs):
        other = (r ^ 1) * rows
        updated = keep_ref[r * rows:(r + 1) * rows] - part_ref[other:other + rows].astype(F32)
        updated = updated.astype(BF)
        if len(out_ref.shape) == 3:
            out_ref[grid_index ^ r] = updated
            continue
        share = out_ref.shape[3]
        for b in range(out_ref.shape[0]):
            out_ref[b, grid_index ^ r] = updated[:, b * share:(b + 1) * share]


def gram_kernel(x_ref, out_ref):
    orbs, rows, lanes = x_ref.shape
    flat = x_ref[...].reshape(orbs * rows, lanes)
    full = lax.dot_general(flat, flat, (((1,), (1,)), ((), ())), preferred_element_type=F32)
    down = lax.broadcasted_iota(jnp.int32, (rows, orbs * rows), 0)
    along = lax.broadcasted_iota(jnp.int32, (rows, orbs * rows), 1)
    same = down == along % rows
    half = [
        jnp.sum(jnp.where(same, full[o * rows:(o + 1) * rows], 0.0), axis=0, keepdims=True)
        for o in range(orbs)
    ]
    half = jnp.concatenate(half, 0)
    gram = jnp.sum(half.T.reshape(orbs, rows, orbs), axis=1)
    deep = orbs * orbs // LANES
    packed = jnp.concatenate([gram[q * deep:(q + 1) * deep] for q in range(orbs // deep)], 1)
    out_ref[...] = jnp.broadcast_to(packed[None], out_ref.shape)


def rotate_kernel(scale, parts_ref, x_ref, out_ref, gram_ref):
    orbs, rows, lanes = x_ref.shape
    packed = jnp.sum(parts_ref[...], axis=0) * scale
    gram = jnp.concatenate(
        [packed[:, q * orbs:(q + 1) * orbs] for q in range(LANES // orbs)], 0)
    gram_ref[...] = gram
    down = lax.broadcasted_iota(jnp.int32, (orbs, orbs), 0)
    along = lax.broadcasted_iota(jnp.int32, (orbs, orbs), 1)
    eye = jnp.where(down == along, 1.0, 0.0)
    zero = jnp.zeros((orbs, LANES - 2 * orbs), F32)
    work = jnp.concatenate([gram, eye, zero], 1)
    row = lax.broadcasted_iota(jnp.int32, (orbs, LANES), 0)
    pivots = jnp.zeros((orbs, LANES), F32)
    for first in range(0, orbs, PANEL):
        columns = [
            jnp.broadcast_to(work[:, c:c + 1], (orbs, LANES)) for c in range(first, first + PANEL)
        ]
        for k in range(first, first + PANEL):
            column = columns[k - first]
            pivot = column[k:k + 1, :]
            pivots = jnp.where(row == k, pivot, pivots)
            factor = jnp.where(row > k, column * (1.0 / pivot), 0.0)
            work = work - factor * work[k:k + 1, :]
            for c in range(k - first + 1, PANEL):
                columns[c] = columns[c] - factor * columns[c][k:k + 1, :]
    work = work * (1.0 / jnp.sqrt(pivots))
    inverse = work[:, orbs:2 * orbs].astype(BF)
    tall = lax.broadcasted_iota(jnp.int32, (orbs * rows, orbs), 0) // rows
    wide = lax.broadcasted_iota(jnp.int32, (orbs * rows, orbs), 1)
    pick = jnp.where(tall == wide, 1.0, 0.0).astype(BF)
    spread = product(pick, inverse).astype(BF)
    spread = lax.dot_general(spread, pick, (((1,), (1,)), ((), ())), preferred_element_type=F32)
    i = lax.broadcasted_iota(jnp.int32, (orbs * rows, 1), 0) % rows
    j = lax.broadcasted_iota(jnp.int32, (1, orbs * rows), 1) % rows
    spread = jnp.where(i == j, spread, 0.0).astype(BF)
    flat = x_ref[...].reshape(orbs * rows, lanes)
    out_ref[...] = product(spread, flat).astype(BF).reshape(orbs, rows, lanes)


def exchanged(x, axis, by, only=None):
    return lax.ppermute(x, axis, [
        (i, i ^ by) for i in range(lax.axis_size(axis)) if only is None or only(i)])


def body(orbitals):
    orb_count, slab_rows, plane_cells = orbitals.shape
    slabs = lax.axis_size("grid")
    blocks = lax.axis_size("blk")
    assert orb_count == slabs == 4 and slab_rows * slabs == NX and blocks % 2 == 0 and STEPS == 2
    top = slabs // 2
    half = orb_count // 2
    core = lax.axis_index("grid") % 2
    even = lax.axis_index("blk") % 2 == 0
    diagonals, weights = make_tables(slab_rows)

    def shifted(x):
        return lax.ppermute(x, "blk", [(i, (i + 2) % blocks) for i in range(blocks)])

    def relayed(mine, received):
        relay = jnp.where(even, mine, received)
        return exchanged(relay, "blk", 1)

    def passed_on(x):
        return exchanged(x, "grid", 1, lambda i: i // 2 == i % 2)

    keep = lax.dynamic_slice_in_dim(orbitals, core * half, half, 0)
    give = lax.dynamic_slice_in_dim(orbitals, (1 - core) * half, half, 0)
    keep, give = lax.optimization_barrier((keep, give))
    held = [keep, exchanged(give, "grid", 1)]
    far = [shifted(held[i]) for i in range(2)]
    across = [exchanged(held[i], "grid", top) for i in range(2)]
    near = [relayed(held[i], far[i]) for i in range(2)]
    far_other = [exchanged(far[0], "grid", top), shifted(across[1])]
    relay, diagonals, weights = lax.optimization_barrier((across[1], diagonals, weights))
    tables = (diagonals, weights)
    near_other = [exchanged(near[0], "grid", top), relayed(relay, far_other[1])]
    local = held + across
    joined = jnp.concatenate([across[1], across[0]], 0)
    passed = [give, passed_on(held[0]), passed_on(joined)]
    acc = add_block(local, passed, far + far_other, tables, None)
    mine, other = add_block(local, passed, near + near_other, tables, acc)
    other = exchanged(other, "grid", 1)
    chunk = plane_cells // blocks
    if chunk % LANES == 0:
        shape = (blocks, slabs, slab_rows, chunk)
    else:
        shape = (slabs, slab_rows, plane_cells)
    updated = pl.pallas_call(
        functools.partial(combine_kernel, slabs),
        out_shape=jax.ShapeDtypeStruct(shape, BF),
        in_specs=[VMEM, VMEM],
        out_specs=VMEM,
        compiler_params=pltpu.CompilerParams(vmem_limit_bytes=SMALL_VMEM),
    )(mine, other)
    if chunk % LANES:
        updated = updated.reshape(slabs, slab_rows, blocks, chunk).transpose(2, 0, 1, 3)
    updated = updated.reshape(blocks * slabs, slab_rows, chunk)
    cellwise = lax.all_to_all(updated, ("blk", "grid"), 0, 0, tiled=True)

    devices = blocks * slabs
    cell_count = NX * NY * NZ
    if devices * slab_rows <= 512 and devices % PANEL == 0 and chunk % LANES == 0:
        local = pl.pallas_call(
            gram_kernel,
            out_shape=jax.ShapeDtypeStruct((devices, devices * devices // LANES, LANES), F32),
            in_specs=[VMEM],
            out_specs=VMEM,
            compiler_params=pltpu.CompilerParams(vmem_limit_bytes=SMALL_VMEM),
        )(cellwise)
        parts = lax.all_to_all(local, ("blk", "grid"), 0, 0, tiled=True)
        return pl.pallas_call(
            functools.partial(rotate_kernel, 1.0 / cell_count),
            out_shape=(
                jax.ShapeDtypeStruct(cellwise.shape, BF),
                jax.ShapeDtypeStruct((devices, devices), F32),
            ),
            in_specs=[VMEM, VMEM],
            out_specs=(VMEM, VMEM),
            compiler_params=pltpu.CompilerParams(vmem_limit_bytes=SMALL_VMEM),
        )(parts, cellwise)
    flat = cellwise.reshape(devices, slab_rows * chunk)
    local = jnp.dot(flat, flat.T, preferred_element_type=F32)
    intersection = lax.psum(local, ("blk", "grid")) / cell_count
    factor = jnp.linalg.cholesky(intersection)
    identity = jnp.eye(devices, dtype=F32)
    inverse = jax.scipy.linalg.solve_triangular(factor, identity, lower=True).astype(BF)
    rotated = product(inverse, flat).astype(BF)
    return (rotated.reshape(cellwise.shape), intersection)


def solution(mesh):
    in_specs = (P("blk", "grid", None),)
    out_specs = (P(None, "grid", "blk"), P())
    return jax.shard_map(body, mesh=mesh, in_specs=in_specs, out_specs=out_specs, check_vma=False)
```
